32 devices in a mesh: gx: 2 (over core), gyz: 16 (over z, y, x).
Axes of the slice: x: 2, y: 2, z: 4, core: 2. Of those that a mesh axis runs over, the one named last changes fastest.
Arguments:
- bands: bfloat16 [16, 80, 40, 512], P('gx', 'gyz'), may hold values from -6 to 6
- potential: float32 [16, 80, 40], P('gx', 'gyz'), may hold values from 0.5 to 4
- eigenvectors: bfloat16 [512, 512], P('gyz'), may hold values from -0.25 to 0.25
Outputs:
- correlation: float32 [512, 512], P('gyz')
- hamiltonian: float32 [512, 512], P('gyz')
- rotated: bfloat16 [16, 80, 40, 512], P('gx', 'gyz')
The draws below stay inside these ranges and needn't reach their ends.
All inputs are finite; a program needn't handle non-finite values.
Results may differ from the reference program's by a relative error of at most 0.0012.
Values may be sent and summed in bfloat16 or wider, within the bound.
A program may use at most 64 MiB of HBM per device.

```python
import math
import jax
import jax.numpy as jnp
from jax import lax

BANDS = 512
CX = 8
CZ = 40
NX = 16
NY = 80


def strengthened(drawn, stream_key, source, target, blocks, factor):
    def block_of(dim):
        return (jnp.arange(drawn.shape[dim]) // (drawn.shape[dim] // blocks)).reshape((-1,) + (1,) * (drawn.ndim - 1 - dim))

    one_side = jax.random.permutation(stream_key, blocks)[block_of(target)]
    other_side = (block_of(target) + blocks // 2) % blocks
    return jnp.where((block_of(source) == one_side) | (block_of(source) == other_side), factor * drawn, drawn)


def levels(rng, dims, pieces, least, largest):
    def one(position, blocks):
        heights = jax.random.uniform(jax.random.fold_in(jax.random.fold_in(rng, 6), position), (blocks,), jnp.float32, least / len(pieces), largest / len(pieces))
        return jnp.repeat(jnp.exp(heights), dims[position] // blocks).reshape((-1,) + (1,) * (len(dims) - position - 1))

    factor_of = one(*pieces[0])
    for cut in pieces[1:]:
        factor_of = factor_of * one(*cut)
    return factor_of


def normal_values(rng, extent, scale, reach, shards=(), held_as=jnp.bfloat16):
    result = jax.random.normal(rng, extent, jnp.float32) * scale
    if len(shards) > 0:
        result = levels(rng, extent, shards, -0.22, 0.18) * result
    return jnp.clip(result, min=-reach, max=reach).astype(held_as)


def bell_draw_with(key, extent, width, bound, pieces, heavy, held_as=jnp.bfloat16):
    entries = width * jax.random.normal(key, extent, jnp.float32)
    if pieces:
        entries = entries * levels(key, extent, pieces, -0.22, 0.18)
    return jnp.clip(strengthened(entries, jax.random.fold_in(key, 3), *heavy), -bound, bound).astype(held_as)


def setup_inputs(seed: int = 0) -> dict:
    streams_of = jax.random.split(jax.random.key(seed), 4)
    bands = bell_draw_with(streams_of[0], (NX, NY, CZ, BANDS), 1.0, 6.0, ((0, 2), (1, 16)), (1, 3, 16, 2.0))
    potential = jnp.clip(jnp.exp(math.log(4.0) - 2.0794415 * jax.random.uniform(streams_of[1], (NX, NY, CZ), jnp.float32) ** levels(streams_of[1], (NX, NY, CZ), ((0, 2), (1, 16)), -0.2, 0.2)), 0.5, 4.0)
    eigenvectors = normal_values(streams_of[2], (BANDS, BANDS), BANDS ** -0.5, 0.25, ((0, 16),))
    return dict(bands=bands, potential=potential, eigenvectors=eigenvectors)


def stencil(padded, potential):
    centre = padded[1:-1, 1:-1, 1:-1].astype(jnp.float32)
    neighbours = padded[2:, 1:-1, 1:-1].astype(jnp.float32) + padded[:-2, 1:-1, 1:-1].astype(jnp.float32)
    neighbours = neighbours + padded[1:-1, 2:, 1:-1].astype(jnp.float32) + padded[1:-1, :-2, 1:-1].astype(jnp.float32)
    neighbours = neighbours + padded[1:-1, 1:-1, 2:].astype(jnp.float32) + padded[1:-1, 1:-1, :-2].astype(jnp.float32)
    return ((3.0 + potential[..., None]) * centre - 0.5 * neighbours).astype(jnp.bfloat16)


def reference(bands, potential, eigenvectors):
    padded = jnp.pad(bands, ((1, 1), (1, 1), (1, 1), (0, 0)))

    def x_plane(plane_index):
        x_slab = lax.dynamic_slice_in_dim(padded, plane_index, 3, 0)
        local_pot = lax.dynamic_slice_in_dim(potential, plane_index, 1, 0)
        return stencil(x_slab, local_pot)[0]

    hamil_bands = lax.map(x_plane, jnp.arange(NX, dtype=jnp.int32))
    cell_count = NX * NY * CZ
    flat_bands = bands.reshape(cell_count, BANDS)
    flat_hamil = hamil_bands.reshape(cell_count, BANDS)
    inv_volume = 1.0 / (CX * NY * CZ)
    correlation = lax.dot_general(flat_bands, flat_bands, (((0,), (0,)), ((), ())), preferred_element_type=jnp.float32) * inv_volume
    hamiltonian = lax.dot_general(flat_bands, flat_hamil, (((0,), (0,)), ((), ())), preferred_element_type=jnp.float32) * inv_volume
    rotated = jnp.dot(flat_bands, eigenvectors, preferred_element_type=jnp.float32).astype(jnp.bfloat16)
    return correlation, hamiltonian, rotated.reshape(bands.shape)
```

```python
import functools
import itertools
import math

import jax
import jax.numpy as jnp
from jax import lax
from jax.experimental import pallas as pl
from jax.experimental.pallas import tpu as pltpu
from jax.sharding import PartitionSpec as P

MESH = pl.DeviceIdType.MESH
F32, BF16 = jnp.float32, jnp.bfloat16
scope = jax.named_scope


def digit_sizes(count):
    sizes, base = [], 2 if count <= 16 else 4
    while count > 1:
        size = base if count % base == 0 else (2 if count % 2 == 0 else count)
        sizes.append(size)
        count //= size
    return tuple(reversed(sizes)) or (1,)


def gram_t(left, right):
    return lax.dot_general(left, right, (((0,), (0,)), ((), ())), preferred_element_type=F32)


class Copies:
    def __init__(self, send_sems, recv_sems):
        self.send_sems, self.recv_sems, self.used = send_sems, recv_sems, 0

    def make(self, src, dst, device_id):
        slot = self.used
        self.used += 1
        return pltpu.make_async_remote_copy(
            src_ref=src, dst_ref=dst, send_sem=self.send_sems.at[slot],
            recv_sem=self.recv_sems.at[slot], device_id=device_id, device_id_type=MESH)


def singles(order):
    return tuple((d,) for d in order)


def plans_of(rows, sizes):
    count = len(sizes)
    if sizes == (2, 2, 2, 2) and rows % 32 == 0:
        ham = ((0, rows // 2, ((2, 3), (0, 1))), (rows // 2, rows, ((0, 1), (2, 3))))
        corr = ((0, rows, ((0, 1), (2, 3))),)
        return ham, corr, ((0, 1), (3,), (2,))
    fast, slow = singles(range(count)[::-1]), singles(range(count))
    return ((0, rows, fast),), ((0, rows, slow),), slow


def peer_count(sizes, group):
    return math.prod(sizes[d] for d in group)


def copies_of(sizes, order):
    return sum(peer_count(sizes, group) - 1 for group in order)


class Stream:
    def __init__(self, context, source, first, last, order, outgoing, received, parts):
        self.context, self.source, self.order, self.outgoing = context, source, order, outgoing
        self.rows, self.received, self.parts = slice(first, last), received, parts
        self.left, self.phase = list(range(len(context[1]))), 0

    def index(self, values):
        at = tuple(values[d] if d in values else slice(None) for d in self.left)
        return at

    def current(self):
        everything = tuple(slice(None) for _ in self.left)
        return self.source[everything + (self.rows,)] if self.phase == 0 else self.source[...]

    def start(self):
        copies, sizes, digits, gx, peer = self.context
        group = self.order[self.phase]
        self.flying = []
        out = self.outgoing[self.phase]
        out[...] = self.current().astype(BF16)
        for k in range(1, peer_count(sizes, group)):
            target, values = peer(group, k)
            copy = copies.make(out.at[self.index(values)],
                               self.received[self.phase].at[k - 1], (gx, target))
            copy.start()
            self.flying.append(copy)

    def finish(self):
        copies, sizes, digits, gx, peer = self.context
        group = self.order[self.phase]
        for copy in self.flying:
            copy.wait_recv()
        own = self.index({d: digits[d] for d in group})
        total = self.source[own + (self.rows,) if self.phase == 0 else own]
        for k in range(1, peer_count(sizes, group)):
            total = total + self.received[self.phase][k - 1].astype(F32)
        self.parts[self.phase][...] = total
        self.source = self.parts[self.phase]
        self.left = [d for d in self.left if d not in group]
        self.phase += 1


def kernel(geometry, grid4, rows_in, pot_in, eig, corr_out, ham_out, rot_out, flat, pot, coef, padded, hq,
           corr, ham, halo_f, halo_b, halo_x, own, ghost, pair_c, pair_h, sum_c, sum_h, gx_c, gx_h,
           send_sems, recv_sems, local_sems, *buffers):
    gx_size, gyz_size, cx, cy, cz, bands, rows, sizes, copy_count = geometry
    ham_plan, corr_plan, coef_plan = plans_of(rows, sizes)
    count = len(sizes)
    half = bands // 2
    gx, gyz = lax.axis_index("gx"), lax.axis_index("gyz")
    parity = lax.rem(gx, 2)
    partner = gx + 1 - 2 * parity
    mine = pl.ds(pl.multiple_of(parity * half, half), half)
    other = pl.ds(pl.multiple_of((1 - parity) * half, half), half)
    strides = []
    step = gyz_size
    for size in sizes:
        step //= size
        strides.append(step)
    digits = [lax.rem(gyz // stride, size) for stride, size in zip(strides, sizes)]
    copies = Copies(send_sems, recv_sems)

    def peer(group, k):
        target, values = gyz, {}
        for d in reversed(group):
            digit = lax.rem(digits[d] + k % sizes[d], sizes[d])
            target = target + (digit - digits[d]) * strides[d]
            values[d] = digit
            k //= sizes[d]
        return target, values

    load_flat = pltpu.make_async_copy(rows_in, flat, local_sems.at[0])
    load_flat.start()
    own_coef = coef.at[tuple(digits) + (slice(None), mine)]
    load_coef = pltpu.make_async_copy(eig.at[:, mine], own_coef, local_sems.at[1])
    load_coef.start()
    load_pot = pltpu.make_async_copy(pot_in, pot, local_sems.at[2])
    load_pot.start()

    barrier = pltpu.get_barrier_semaphore()
    first_x, last_x, first_y, last_y = gx == 0, gx == gx_size - 1, gyz == 0, gyz == gyz_size - 1
    beside = ((first_x, (gx - 1, gyz)), (last_x, (gx + 1, gyz)), (first_y, (gx, gyz - 1)), (last_y, (gx, gyz + 1)))
    for edge, device in beside:
        @pl.when(jnp.logical_not(edge))
        def _():
            pl.semaphore_signal(barrier, inc=1, device_id=device, device_id_type=MESH)
    neighbours = sum(1 - edge.astype(jnp.int32) for edge, _ in beside)
    greeted = []
    groups = []
    for _, _, order in ham_plan + corr_plan + ((0, 0, coef_plan),):
        groups += [group for group in order if group not in groups]
    wide = [group for group in groups if not any(set(group) < set(other) for other in groups)]
    for group in wide:
        greeted += [(gx, peer(group, k)[0]) for k in range(1, peer_count(sizes, group))]
    greeted += [(lax.rem(gx + 2 * k, gx_size), gyz) for k in range(1, gx_size // 2)]
    for device in greeted:
        pl.semaphore_signal(barrier, inc=1, device_id=device, device_id_type=MESH)
    with scope("barrier"):
        pl.semaphore_wait(barrier, len(greeted) + neighbours)

    sent = []

    def coef_phase(at):
        started = []
        done = {d for group in coef_plan[:at] for d in group}
        index = tuple(slice(None) if d in done else digits[d] for d in range(count)) + (slice(None), mine)
        for k in range(1, peer_count(sizes, coef_plan[at])):
            block = coef.at[index]
            copy = copies.make(block, block, (gx, peer(coef_plan[at], k)[0]))
            copy.start()
            started.append(copy)
        sent.extend(started)
        return started

    def next_coef_phase(started, at):
        for copy in started:
            copy.wait_recv()
        return coef_phase(at) if at < len(coef_plan) else []


    to_x = copies.make(grid4.at[cx - 1], halo_x, (lax.rem(gx + 1, gx_size), gyz))
    cut_x = (cx + 1) // 2
    ahead = copies.make(grid4.at[:cut_x, cy - 1], halo_f, (gx, lax.rem(gyz + 1, gyz_size)))
    back = copies.make(grid4.at[cut_x:, 0], halo_b, (gx, lax.rem(gyz + gyz_size - 1, gyz_size)))

    @pl.when(jnp.logical_not(last_y))
    def _():
        ahead.start()

    @pl.when(jnp.logical_not(first_y))
    def _():
        back.start()

    @pl.when(jnp.logical_not(last_x))
    def _():
        to_x.start()

    @pl.when(first_x)
    def _():
        halo_x[...] = jnp.zeros_like(halo_x)

    @pl.when(first_y)
    def _():
        halo_f[...] = jnp.zeros_like(halo_f)

    @pl.when(last_y)
    def _():
        halo_b[...] = jnp.zeros_like(halo_b)

    load_coef.wait()
    coef_copies = coef_phase(0)

    def block_index(block):
        index = []
        for stride in strides:
            index.append(block // stride)
            block %= stride
        return tuple(index)

    def store_rows(target, first, value):
        for j in range(value.shape[0] // rows):
            target[block_index(first // rows + j)] = value[j * rows:(j + 1) * rows]

    tile = min(bands, 256)
    with scope('load'):
        load_flat.wait()
    for first in range(0, bands, tile):
        store_rows(corr, first, gram_t(flat[:, first:first + tile], flat[...]))
    everything = tuple([slice(None)] * (count + 1))
    pair_copy_c = copies.make(corr.at[everything + (other,)], pair_c, (partner, gyz))
    pair_copy_c.start()
    load_pot.wait()

    plane = cy * cz
    cells = cx * plane
    chunk = 2 * cz if cells % (2 * cz) == 0 else cz
    for first in range(0, cells, chunk):
        padded[first:first + chunk] = flat[first:first + chunk].astype(F32)
    row = lax.broadcasted_iota(jnp.int32, (cz, cz), 0)
    column = lax.broadcasted_iota(jnp.int32, (cz, cz), 1)
    zero_row = jnp.zeros((1, bands), F32)

    def segment(x, y):
        at = x * plane + y * cz
        centre = padded[at:at + cz]
        near = jnp.concatenate([zero_row, centre[:-1]]) + jnp.concatenate([centre[1:], zero_row])
        for there, offset in ((x > 0, -plane), (x < cx - 1, plane), (y > 0, -cz), (y < cy - 1, cz)):
            if there:
                near = near + padded[at + offset:at + offset + cz]
        local = jnp.broadcast_to(pot[y, x:x + 1, :], (cz, cz))
        factor = 3.0 + jnp.sum(jnp.where(row == column, local, 0.0), axis=1, keepdims=True)
        return factor * centre - 0.5 * near

    order = list(itertools.product(range(cx), range(cy)))
    per = chunk // cz
    for first in range(0, len(order), per):
        hq[first * cz:(first + per) * cz] = jnp.concatenate(
            [segment(*xy) for xy in order[first:first + per]]).astype(BF16)

    context = (copies, sizes, digits, gx, peer)
    taken = iter(buffers)

    def streams(plan, source):
        made = []
        for first, last, digit_order in plan:
            outgoing = [next(taken) for _ in digit_order]
            received = [next(taken) for _ in digit_order]
            parts = [next(taken) for _ in digit_order]
            made.append(Stream(context, source, first, last, digit_order, outgoing, received, parts))
        return made

    ham_streams, corr_streams = streams(ham_plan, sum_h), streams(corr_plan, sum_c)

    def begin(group):
        for stream in group:
            stream.start()

    def end(group):
        for stream in group:
            stream.finish()
            sent.extend(stream.flying)
            if stream.phase < len(stream.order):
                stream.start()

    with scope('pair_c'):
        pair_copy_c.wait_recv()
    sum_c[...] = corr[everything + (mine,)] + pair_c[...]
    begin(corr_streams)

    for first in range(0, bands, tile):
        store_rows(ham, first, gram_t(flat[:, first:first + tile], hq[...]))

    own[...] = jnp.concatenate(
        [flat[x * plane:x * plane + cz] for x in range(cut_x)]
        + [flat[x * plane + plane - cz:x * plane + plane] for x in range(cut_x, cx)] + [flat[0:plane]])

    with scope('halo'):
        @pl.when(jnp.logical_not(first_y))
        def _():
            ahead.wait_recv()

        @pl.when(jnp.logical_not(last_y))
        def _():
            back.wait_recv()

        @pl.when(jnp.logical_not(first_x))
        def _():
            to_x.wait_recv()

    with scope('coef_z'):
        coef_copies = next_coef_phase(coef_copies, 1)

    ghost[...] = jnp.concatenate(
        [halo_f[x] for x in range(cut_x)] + [halo_b[x] for x in range(cx - cut_x)]
        + [halo_x[y] for y in range(cy)])
    cross = padded.at[0:bands]
    for first in range(0, bands, tile):
        cut = slice(first, first + tile)
        cross[cut] = -0.5 * gram_t(own[:, cut], ghost[...])
    for first in range(0, bands, tile):
        cut = slice(first, first + tile)
        value = cross[cut] + jnp.transpose(cross[:, cut])
        for j in range(tile // rows):
            index = block_index(first // rows + j)
            ham[index] = ham[index] + value[j * rows:(j + 1) * rows]
    pair_copy_h = copies.make(ham.at[everything + (other,)], pair_h, (partner, gyz))
    pair_copy_h.start()
    with scope('pair_h'):
        pair_copy_h.wait_recv()
    sum_h[...] = ham[everything + (mine,)] + pair_h[...]
    begin(ham_streams)

    scale = 1.0 / (cells * gyz_size)

    def last_sum(group, gx_recv, final):
        for at, stream in enumerate(group):
            final[stream.rows, mine] = stream.source[...]
        others = []
        for k in range(1, gx_size // 2):
            target = (lax.rem(gx + 2 * k, gx_size), gyz)
            copy = copies.make(final.at[:, mine], gx_recv.at[k - 1], target)
            copy.start()
            others.append(copy)
        for copy in others:
            copy.wait()
        total = final[:, mine]
        for k in range(1, gx_size // 2):
            total = total + gx_recv[k - 1]
        final[:, mine] = total * scale
        copy = copies.make(final.at[:, mine], final.at[:, mine], (partner, gyz))
        copy.start()
        return copy

    coef_steps = len(coef_plan)
    with scope('corr_1'):
        end(corr_streams)
    with scope('coef_x'):
        if coef_steps > 2:
            coef_copies = next_coef_phase(coef_copies, 2)
    with scope('ham_1'):
        end(ham_streams)
    with scope('coef_y'):
        for at in range(min(coef_steps, 3), coef_steps + 1):
            coef_copies = next_coef_phase(coef_copies, at)
    mine_block = coef.at[everything + (mine,)]
    pair_copy_e = copies.make(mine_block, mine_block, (partner, gyz))
    pair_copy_e.start()
    with scope('corr_2'):
        while corr_streams[0].phase < len(corr_plan[0][2]):
            end(corr_streams)
    last_c = last_sum(corr_streams, gx_c, corr_out)
    with scope('pair_e'):
        pair_copy_e.wait_recv()
    whole = coef[...].reshape(bands, bands)
    part = max(size for size in range(16, 512, 16) if cells % size == 0)
    for first in range(0, cells, part):
        rot_out[first:first + part] = jnp.dot(
            flat[first:first + part], whole, preferred_element_type=F32).astype(BF16)

    with scope('ham_2'):
        while ham_streams[0].phase < len(ham_plan[0][2]):
            end(ham_streams)
    last_h = last_sum(ham_streams, gx_h, ham_out)

    with scope('last'):
        last_c.wait_recv()
        last_h.wait_recv()
    for copy in sent + [pair_copy_c, pair_copy_h, pair_copy_e, last_c, last_h]:
        copy.wait_send()

    @pl.when(jnp.logical_not(last_y))
    def _():
        ahead.wait_send()

    @pl.when(jnp.logical_not(first_y))
    def _():
        back.wait_send()

    @pl.when(jnp.logical_not(last_x))
    def _():
        to_x.wait_send()

    assert copies.used == copy_count


def deliver(corr, ham, rot, corr_out, ham_out, rot_out, sems):
    copies = [pltpu.make_async_copy(source, target, sems.at[i]) for i, (source, target) in
              enumerate(((rot, rot_out), (corr, corr_out), (ham, ham_out)))]
    for copy in copies:
        copy.start()
    for copy in copies:
        copy.wait()


def in_hbm(array):
    return pltpu.with_memory_space_constraint(array, pltpu.HBM)


def on_device(bands, potential, eigenvectors):
    gx_size, gyz_size = lax.axis_size("gx"), lax.axis_size("gyz")
    cx, cy, cz, width = bands.shape
    rows = eigenvectors.shape[0]
    cells = cx * cy * cz
    sizes = digit_sizes(gyz_size)
    count = len(sizes)
    half = width // 2
    flat = bands.reshape(cells, width)
    ham_plan, corr_plan, coef_plan = plans_of(rows, sizes)
    orders = [order for _, _, order in ham_plan + corr_plan] + [coef_plan]
    copy_count = 3 + sum(copies_of(sizes, order) for order in orders) + 3 + 2 * (gx_size // 2)
    geometry = (gx_size, gyz_size, cx, cy, cz, width, rows, sizes, copy_count)

    buffers = []
    for first, last, order in ham_plan + corr_plan:
        outgoing, received, parts, left = [], [], [], list(range(count))
        for group in order:
            outgoing.append(pltpu.VMEM(tuple(sizes[i] for i in left) + (last - first, half), BF16))
            left = [d for d in left if d not in group]
            shape = tuple(sizes[i] for i in left) + (last - first, half)
            received.append(pltpu.VMEM((peer_count(sizes, group) - 1,) + shape, BF16))
            parts.append(pltpu.VMEM(shape, F32))
        buffers += outgoing + received + parts

    cut_x = (cx + 1) // 2
    ghosts = (cx + cy) * cz
    wide, narrow = sizes + (rows, width), sizes + (rows, half)
    others = max(gx_size // 2 - 1, 1)
    vmem, anywhere = pl.BlockSpec(memory_space=pltpu.VMEM), pl.BlockSpec(memory_space=pl.ANY)
    results = (jax.ShapeDtypeStruct((rows, width), F32), jax.ShapeDtypeStruct((rows, width), F32),
               jax.ShapeDtypeStruct((cells, width), BF16))
    computed = pl.pallas_call(
        functools.partial(kernel, geometry),
        out_shape=results,
        in_specs=[pl.BlockSpec(memory_space=pltpu.HBM)] * 4,
        out_specs=(vmem, vmem, vmem),
        scratch_shapes=[
            pltpu.VMEM((cells, width), BF16), pltpu.VMEM((cy, cx, cz), F32),
            pltpu.VMEM(wide, BF16),
            pltpu.VMEM((cells, width), F32), pltpu.VMEM((cells, width), BF16),
            pltpu.VMEM(wide, F32), pltpu.VMEM(wide, F32),
            pltpu.VMEM((cut_x, cz, width), BF16), pltpu.VMEM((cx - cut_x, cz, width), BF16),
            pltpu.VMEM((cy, cz, width), BF16),
            pltpu.VMEM((ghosts, width), BF16), pltpu.VMEM((ghosts, width), BF16),
            pltpu.VMEM(narrow, F32), pltpu.VMEM(narrow, F32),
            pltpu.VMEM(narrow, F32), pltpu.VMEM(narrow, F32),
            pltpu.VMEM((others, rows, half), F32), pltpu.VMEM((others, rows, half), F32),
            pltpu.SemaphoreType.DMA((copy_count,)), pltpu.SemaphoreType.DMA((copy_count,)),
            pltpu.SemaphoreType.DMA((3,)), *buffers,
        ],
        compiler_params=pltpu.CompilerParams(
            collective_id=0, has_side_effects=True, vmem_limit_bytes=52 * 1024 * 1024),
    )(bands, flat, in_hbm(jnp.transpose(potential, (1, 0, 2))), in_hbm(eigenvectors))
    corr, ham, rotated = pl.pallas_call(
        deliver, out_shape=results, in_specs=[vmem] * 3, out_specs=[anywhere] * 3,
        scratch_shapes=[pltpu.SemaphoreType.DMA((3,))],
        compiler_params=pltpu.CompilerParams(vmem_limit_bytes=8 * 1024 * 1024),
    )(*computed)
    return corr, ham, rotated.reshape(bands.shape)


def solution(mesh):
    in_specs = (P("gx", "gyz", None, None), P("gx", "gyz", None), P("gyz", None))
    out_specs = (P("gyz", None), P("gyz", None), P("gx", "gyz", None, None))
    return jax.shard_map(
        on_device, mesh=mesh, in_specs=in_specs, out_specs=out_specs, check_vma=False
    )
```

```python
import functools
import itertools
import math
import types

import jax
import jax.numpy as jnp
from jax import lax
from jax.experimental import pallas as pl
from jax.experimental.pallas import tpu as pltpu
from jax.sharding import PartitionSpec as P

MESH = pl.DeviceIdType.MESH
F32, BF16 = jnp.float32, jnp.bfloat16
scope = jax.named_scope


def digit_sizes(count):
    sizes, base = [], 2 if count <= 16 else 4
    while count > 1:
        size = base if count % base == 0 else (2 if count % 2 == 0 else count)
        sizes.append(size)
        count //= size
    return tuple(reversed(sizes)) or (1,)


def gram_t(left, right):
    return lax.dot_general(left, right, (((0,), (0,)), ((), ())), preferred_element_type=F32)


class Group:
    def __init__(self, send_sem, recv_sem):
        self.send_sem, self.recv_sem, self.whole = send_sem, recv_sem, None

    def start(self, src, dst, device_id):
        pltpu.make_async_remote_copy(
            src_ref=src, dst_ref=dst, send_sem=self.send_sem, recv_sem=self.recv_sem,
            device_id=device_id, device_id_type=MESH).start()

    def wait_recv(self):
        pltpu.make_async_copy(self.whole, self.whole, self.recv_sem).wait()

    def wait_send(self):
        pltpu.make_async_copy(self.whole, self.whole, self.send_sem).wait()


class Copies:
    def __init__(self, send_sems, recv_sems):
        self.send_sems, self.recv_sems, self.used = send_sems, recv_sems, 0

    def slot(self):
        self.used += 1
        return self.send_sems.at[self.used - 1], self.recv_sems.at[self.used - 1]

    def make(self, src, dst, device_id):
        send_sem, recv_sem = self.slot()
        return pltpu.make_async_remote_copy(
            src_ref=src, dst_ref=dst, send_sem=send_sem, recv_sem=recv_sem,
            device_id=device_id, device_id_type=MESH)

    def group(self, whole):
        made = Group(*self.slot())
        made.whole = whole
        return made


Z, XY = (0, 1), (2, 3)


def singles(order):
    return tuple((d,) for d in order)


def plans_of(rows, sizes):
    count = len(sizes)
    if sizes == (2, 2, 2, 2) and rows % 32 == 0:
        ham = ((0, rows // 2, (XY, Z)), (rows // 2, rows, (Z, XY)))
        return ham, ((0, rows, (Z, XY)),), (Z, (3,), (2,))
    fast, slow = singles(range(count)[::-1]), singles(range(count))
    return ((0, rows, fast),), ((0, rows, slow),), slow


def peer_count(sizes, group):
    return math.prod(sizes[d] for d in group)


def copies_of(sizes, order):
    return sum(peer_count(sizes, group) - 1 for group in order)


class Stream:
    def __init__(self, context, source, final, first, last, order, buffers):
        self.context, self.source, self.final, self.order = context, source, final, order
        self.rows, self.buffers = slice(first, last), buffers
        self.left, self.phase = list(range(len(context.sizes))), 0

    def index(self, values):
        return tuple(values[d] if d in values else slice(None) for d in self.left)

    def peers(self):
        group = self.order[self.phase]
        return [self.context.peer(group, k) for k in range(peer_count(self.context.sizes, group))]

    def combos(self, fixed):
        free = [d for d in self.left if d not in fixed]
        for values in itertools.product(*(range(self.context.sizes[d]) for d in free)):
            yield {**dict(zip(free, values)), **fixed}

    def diagonal(self, values, parity):
        ctx = self.context
        block = sum(values.get(d, ctx.digits[d]) * ctx.strides[d] for d in range(len(ctx.sizes)))
        shape = (self.rows.stop - self.rows.start, ctx.half)
        row = lax.broadcasted_iota(jnp.int32, shape, 0) + (block * ctx.rows + self.rows.start)
        return row == lax.broadcasted_iota(jnp.int32, shape, 1) + parity * ctx.half

    def round(self, fixed):
        out, extra = self.buffers[self.phase][:2]
        for values in self.combos(fixed):
            at = self.index(values)
            value = self.source[at + (self.rows,) if self.phase == 0 else at]
            short = value.astype(BF16)
            out[at] = short
            rest = jnp.where(self.diagonal(values, self.context.parity), value - short.astype(F32), 0.0)
            extra[at] = jnp.sum(rest, axis=0, keepdims=True)

    def open(self):
        landing, extras = self.buffers[self.phase][2:4]
        self.flights = self.context.copies.group(landing), self.context.copies.group(extras)

    def ship(self, at, slot, device):
        out, extra, landing, extras = self.buffers[self.phase][:4]
        self.flights[0].start(out.at[at], landing.at[slot], device)
        self.flights[1].start(extra.at[at], extras.at[slot], device)

    def send(self, k):
        target, values = self.peers()[k]
        self.round(values)
        self.ship(self.index(values), k - 1, (self.context.gx, target))

    def start(self):
        self.open()
        for k in range(1, len(self.peers())):
            self.send(k)

    def start_both(self):
        self.open()
        self.round({})
        peers = self.peers()
        for k, (target, values) in enumerate(peers):
            at = self.index(values)
            if k:
                self.ship(at, k - 1, (self.context.gx, target))
            self.ship(at, len(peers) - 1 + k, (self.context.partner, target))

    def land(self):
        for flight in self.flights:
            flight.wait_recv()

    def finish_both(self, columns, scale):
        self.land()
        out, extra, landing, extras = self.buffers[self.phase][:4]
        many = len(self.peers())
        at = self.index(self.peers()[0][1])
        mine = [(out[at], extra[at])] + [(landing[k], extras[k]) for k in range(many - 1)]
        across = [(landing[k], extras[k]) for k in range(many - 1, 2 * many - 1)]
        parity = self.context.parity
        for column, side, parts in zip(columns, (parity, 1 - parity), (mine, across)):
            total = sum(part.astype(F32) for part, _ in parts)
            rest = sum(rest for _, rest in parts)
            total = total + jnp.where(self.diagonal({}, side), rest, 0.0)
            self.final[self.rows, column] = total * scale
        self.phase += 1

    def finish(self):
        self.land()
        _, _, landing, extras, result = self.buffers[self.phase]
        own = self.peers()[0][1]
        for values in self.combos(own):
            at = self.index(values)
            total = self.source[at + (self.rows,) if self.phase == 0 else at]
            keep = tuple(values[d] for d in self.left if d not in own)
            rest = 0.0
            for k in range(landing.shape[0]):
                total = total + landing[(k,) + keep].astype(F32)
                rest = rest + extras[(k,) + keep]
            result[keep + (Ellipsis,)] = total + jnp.where(self.diagonal(values, self.context.parity), rest, 0.0)
        self.source = result
        self.left = [d for d in self.left if d not in own]
        self.phase += 1


def kernel(geometry, grid4, rows_in, pot_in, eig, corr_out, ham_out, rot_out, flat, pot, coef, padded, hq,
           corr, ham, halo_f, halo_b, halo_x, face, turned, ghosts, late, pair_l, pair_c, pair_h, sum_c, sum_h, gx_c, gx_h,
           send_sems, recv_sems, local_sems, *buffers):
    gx_size, gyz_size, cx, cy, cz, bands, rows, sizes, copy_count = geometry
    ham_plan, corr_plan, coef_plan = plans_of(rows, sizes)
    count = len(sizes)
    half = bands // 2
    relayed, direct = sizes == (2, 2, 2, 2), gx_size == 2
    gx, gyz = lax.axis_index("gx"), lax.axis_index("gyz")
    parity = lax.rem(gx, 2)
    partner = gx + 1 - 2 * parity
    mine = pl.ds(pl.multiple_of(parity * half, half), half)
    other = pl.ds(pl.multiple_of((1 - parity) * half, half), half)
    strides = []
    step = gyz_size
    for size in sizes:
        step //= size
        strides.append(step)
    digits = [lax.rem(gyz // stride, size) for stride, size in zip(strides, sizes)]
    copies = Copies(send_sems, recv_sems)

    def peer(group, k):
        target, values = gyz, {}
        for d in reversed(group):
            digit = lax.rem(digits[d] + k % sizes[d], sizes[d])
            target = target + (digit - digits[d]) * strides[d]
            values[d] = digit
            k //= sizes[d]
        return target, values

    load_flat = pltpu.make_async_copy(rows_in, flat, local_sems.at[0])
    load_flat.start()
    own_coef = coef.at[tuple(digits) + (slice(None), mine)]
    load_coef = pltpu.make_async_copy(eig.at[:, mine], own_coef, local_sems.at[1])
    load_coef.start()
    load_pot = pltpu.make_async_copy(pot_in, pot, local_sems.at[2])
    load_pot.start()

    barrier = pltpu.get_barrier_semaphore()
    first_x, last_x, first_y, last_y = gx == 0, gx == gx_size - 1, gyz == 0, gyz == gyz_size - 1
    beside = ((first_x, (gx - 1, gyz)), (last_x, (gx + 1, gyz)), (first_y, (gx, gyz - 1)), (last_y, (gx, gyz + 1)))
    for edge, device in beside:
        @pl.when(jnp.logical_not(edge))
        def _():
            pl.semaphore_signal(barrier, inc=1, device_id=device, device_id_type=MESH)
    neighbours = sum(1 - edge.astype(jnp.int32) for edge, _ in beside)
    greeted = []
    if direct:
        for group in sorted({order[-1] for _, _, order in ham_plan + corr_plan}):
            greeted += [(partner, peer(group, k)[0]) for k in range(1, peer_count(sizes, group))]
    groups = []
    for _, _, order in ham_plan + corr_plan + ((0, 0, coef_plan),):
        groups += [group for group in order if group not in groups]
    wide = [group for group in groups if not any(set(group) < set(other) for other in groups)]
    for group in wide:
        greeted += [(gx, peer(group, k)[0]) for k in range(1, peer_count(sizes, group))]
    greeted += [(lax.rem(gx + 2 * k, gx_size), gyz) for k in range(1, gx_size // 2)]
    for device in greeted:
        pl.semaphore_signal(barrier, inc=1, device_id=device, device_id_type=MESH)
    with scope("barrier"):
        pl.semaphore_wait(barrier, len(greeted) + neighbours)

    sent = []

    def coef_send(group, held):
        started = []
        for k in range(1, peer_count(sizes, group)):
            block = coef.at[held + (slice(None), mine)]
            started.append(copies.make(block, block, (gx, peer(group, k)[0])))
            started[-1].start()
        sent.extend(started)
        return started

    def coef_held(groups):
        done = {d for group in groups for d in group}
        return tuple(slice(None) if d in done else digits[d] for d in range(count))

    def coef_exchange():
        block = coef.at[tuple([slice(None)] * (count + 1)) + (mine,)]
        coef_state[2] = copies.make(block, block, (partner, gyz))
        coef_state[2].start()

    def coef_wait(flying):
        for copy in flying:
            copy.wait_recv()

    def coef_start():
        coef_state[1] = coef_send(coef_plan[0], coef_held(()))

    coef_steps = 4 if relayed else len(coef_plan)

    def coef_step():
        state, at = coef_state, coef_state[0]
        state[0] += 1
        with scope("coef_%d" % at):
            if not relayed:
                coef_wait(state[1])
                if at + 1 < len(coef_plan):
                    state[1] = coef_send(coef_plan[at + 1], coef_held(coef_plan[:at + 1]))
                else:
                    coef_exchange()
                return
            held = coef_held(coef_plan[:-2])
            if at == 0:
                coef_wait(state[1])
                state[3] = coef_send(coef_plan[-1], held)
            elif at == 1:
                state[1] = coef_send(coef_plan[-2], held)
            elif at == 2:
                coef_wait(state[1])
                d, = coef_plan[-2]
                state[3] += coef_send(coef_plan[-1], held[:d] + (1 - digits[d],) + held[d + 1:])
            else:
                coef_wait(state[3])
                coef_exchange()

    coef_state = [0, None, None, []]
    load_coef.wait()

    to_x = copies.make(grid4.at[cx - 1], halo_x, (lax.rem(gx + 1, gx_size), gyz))
    cut_x = (cx + 1) // 2
    ahead = copies.make(grid4.at[:cut_x, cy - 1], halo_f, (gx, lax.rem(gyz + 1, gyz_size)))
    back = copies.make(grid4.at[cut_x:, 0], halo_b, (gx, lax.rem(gyz + gyz_size - 1, gyz_size)))

    @pl.when(jnp.logical_not(last_y))
    def _():
        ahead.start()

    @pl.when(jnp.logical_not(first_y))
    def _():
        back.start()

    @pl.when(jnp.logical_not(last_x))
    def _():
        to_x.start()

    @pl.when(first_x)
    def _():
        halo_x[...] = jnp.zeros_like(halo_x)

    @pl.when(first_y)
    def _():
        halo_f[...] = jnp.zeros_like(halo_f)

    @pl.when(last_y)
    def _():
        halo_b[...] = jnp.zeros_like(halo_b)

    coef_start()

    def block_index(block):
        index = []
        for stride in strides:
            index.append(block // stride)
            block %= stride
        return tuple(index)

    def store_rows(target, first, value):
        for j in range(value.shape[0] // rows):
            target[block_index(first // rows + j)] = value[j * rows:(j + 1) * rows]

    tile = min(bands, 256)
    with scope('load'):
        load_flat.wait()
    for first in range(0, bands, tile):
        store_rows(corr, first, gram_t(flat[:, first:first + tile], flat[...]))
    everything = tuple([slice(None)] * (count + 1))
    pair_copy_c = copies.make(corr.at[everything + (other,)], pair_c, (partner, gyz))
    pair_copy_c.start()
    load_pot.wait()

    plane = cy * cz
    cells = cx * plane
    chunk = 2 * cz if cells % (2 * cz) == 0 else cz
    for first in range(0, cells, chunk):
        padded[first:first + chunk] = flat[first:first + chunk].astype(F32)
    row = lax.broadcasted_iota(jnp.int32, (cz, cz), 0)
    column = lax.broadcasted_iota(jnp.int32, (cz, cz), 1)
    zero_row = jnp.zeros((1, bands), F32)

    def segment(x, y):
        at = x * plane + y * cz
        centre = padded[at:at + cz]
        near = jnp.concatenate([zero_row, centre[:-1]]) + jnp.concatenate([centre[1:], zero_row])
        for there, offset in ((x > 0, -plane), (x < cx - 1, plane), (y > 0, -cz), (y < cy - 1, cz)):
            if there:
                near = near + padded[at + offset:at + offset + cz]
        local = jnp.broadcast_to(pot[y, x:x + 1, :], (cz, cz))
        factor = 3.0 + jnp.sum(jnp.where(row == column, local, 0.0), axis=1, keepdims=True)
        return factor * centre - 0.5 * near

    order = list(itertools.product(range(cx), range(cy)))
    per = chunk // cz
    for first in range(0, len(order), per):
        hq[first * cz:(first + per) * cz] = jnp.concatenate(
            [segment(*xy) for xy in order[first:first + per]]).astype(BF16)

    context = types.SimpleNamespace(
        copies=copies, sizes=sizes, digits=digits, strides=strides, peer=peer, gx=gx, partner=partner,
        parity=parity, rows=rows, half=half)
    taken = iter(buffers)

    scale = 1.0 / (cells * gyz_size)

    def streams(plan, source, final):
        return [Stream(context, source, final, first, last, order, [[next(taken) for _ in range(5)] for _ in order])
                for first, last, order in plan]

    ham_streams, corr_streams = streams(ham_plan, sum_h, ham_out), streams(corr_plan, sum_c, corr_out)

    def begin(group):
        for stream in group:
            stream.start()

    def end(group):
        for stream in group:
            if direct and stream.phase == len(stream.order) - 1:
                stream.finish_both((mine, other), scale)
                sent.extend(stream.flights)
                continue
            stream.finish()
            sent.extend(stream.flights)
            if direct and stream.phase == len(stream.order) - 1:
                stream.start_both()
            elif stream.phase < len(stream.order):
                stream.start()

    with scope('pair_c'):
        pair_copy_c.wait_recv()
    sum_c[...] = corr[everything + (mine,)] + pair_c[...]
    begin(corr_streams)

    def corr_step():
        at = corr_streams[0].phase
        with scope("corr_%d" % at):
            end(corr_streams)

    for first in range(0, bands, tile):
        store_rows(ham, first, gram_t(flat[:, first:first + tile], hq[...]))

    def add_cross(target, column, value):
        for j in range(bands // rows):
            index = block_index(j) + (slice(None), column)
            target[index] = target[index] - 0.5 * value[j * rows:(j + 1) * rows]

    faces = []
    for at, (cells_x, y) in enumerate(((range(cut_x), 0), (range(cut_x, cx), cy - 1))):
        own = jnp.concatenate([flat[x * plane + y * cz:x * plane + y * cz + cz] for x in cells_x])
        face[at, 0:own.shape[0]] = own
        turned[at, :, 0:own.shape[0]] = jnp.transpose(own)
        faces.append((face.at[at, 0:own.shape[0]], turned.at[at, :, 0:own.shape[0]]))

    @pl.when(jnp.logical_not(first_x))
    def _():
        to_x.wait_recv()

    near, far = flat[0:plane], jnp.concatenate([halo_x[y] for y in range(cy)])
    for first in range(0, bands, tile):
        cut = slice(first, first + tile)
        add_cross(ham, cut, gram_t(near, far[:, cut]) + gram_t(far, near[:, cut]))

    with scope('ahead'):
        @pl.when(jnp.logical_not(first_y))
        def _():
            ahead.wait_recv()

    ghosts[0:cut_x * cz] = jnp.concatenate([halo_f[x] for x in range(cut_x)])
    forward = ghosts.at[0:cut_x * cz]
    forward_t = jnp.transpose(forward[...])
    backward = ghosts.at[cut_x * cz:cx * cz]

    def cross(at, ghost, ghost_t, column):
        near, near_t = faces[at]
        return (jnp.dot(near_t[...], ghost[:, column], preferred_element_type=F32)
                + jnp.dot(ghost_t, near[:, column], preferred_element_type=F32))

    def add(column, value):
        add_cross(ham, column, value)

    add(other, cross(0, forward, forward_t, other))
    pair_copy_h = copies.make(ham.at[everything + (other,)], pair_h, (partner, gyz))
    pair_copy_h.start()
    add(mine, cross(0, forward, forward_t, mine))

    if coef_state[0] < coef_steps:
        coef_step()
    with scope('back'):
        @pl.when(jnp.logical_not(last_y))
        def _():
            back.wait_recv()

    if coef_state[0] < coef_steps:
        coef_step()
    ghosts[cut_x * cz:cx * cz] = jnp.concatenate([halo_b[x] for x in range(cx - cut_x)])
    backward_t = jnp.transpose(backward[...])
    value = cross(1, backward, backward_t, other)
    for j in range(bands // rows):
        late[block_index(j)] = (-0.5 * value[j * rows:(j + 1) * rows]).astype(BF16)
    pieces = [(ham_streams[0], k, at) for k, at in enumerate(ham_streams[0].index(values) for _, values in ham_streams[0].peers())]
    pieces = pieces[1:] + [(stream, None, everything[:-1]) for stream in ham_streams[1:]] + pieces[:1]
    pair_copies_h = []
    for stream, k, at in pieces:
        at = at + (stream.rows,)
        copy = copies.make(late.at[at], pair_l.at[at], (partner, gyz))
        copy.start()
        pair_copies_h.append(copy)
    add(mine, cross(1, backward, backward_t, mine))
    with scope('pair_h'):
        ham_streams[0].open()
        pair_copy_h.wait_recv()
        for (stream, k, at), copy in zip(pieces, pair_copies_h):
            at = at + (stream.rows,)
            copy.wait_recv()
            sum_h[at] = ham[at + (mine,)] + pair_h[at] + pair_l[at].astype(F32)
            if k is None:
                stream.start()
            elif k:
                stream.send(k)

    def last_sum(group, gx_recv, final):
        for at, stream in enumerate(group):
            final[stream.rows, mine] = stream.source[...]
        others = []
        for k in range(1, gx_size // 2):
            target = (lax.rem(gx + 2 * k, gx_size), gyz)
            copy = copies.make(final.at[:, mine], gx_recv.at[k - 1], target)
            copy.start()
            others.append(copy)
        for copy in others:
            copy.wait()
        total = final[:, mine]
        for k in range(1, gx_size // 2):
            total = total + gx_recv[k - 1]
        final[:, mine] = total * scale
        copy = copies.make(final.at[:, mine], final.at[:, mine], (partner, gyz))
        copy.start()
        return copy

    part = max(size for size in range(16, 512, 16) if cells % size == 0)

    def rotate(column):
        some = coef[everything + (column,)].reshape(bands, half)
        for first in range(0, cells, part):
            rot_out[first:first + part, column] = jnp.dot(
                flat[first:first + part], some, preferred_element_type=F32).astype(BF16)

    last = []
    if relayed:
        steps = ["corr", "coef", "ham", "coef", "rot", "corr", "ham"]
    else:
        steps = ["coef"] * (coef_steps - coef_state[0]) + ["rot"]
        steps += ["corr"] * len(corr_plan[0][2]) + ["ham"] * len(ham_plan[0][2])
    for step in steps:
        if step == "corr":
            corr_step()
            if corr_streams[0].phase == len(corr_streams[0].order):
                last += [] if direct else [last_sum(corr_streams, gx_c, corr_out)]
        if step == "ham":
            at = ham_streams[0].phase
            with scope("ham_%d" % at):
                for stream in ham_streams:
                    end([stream])
            if ham_streams[0].phase == len(ham_streams[0].order):
                last += [] if direct else [last_sum(ham_streams, gx_h, ham_out)]
        if step == "coef":
            coef_step()
        if step == "rot":
            rotate(mine)
            with scope("pair_e"):
                coef_state[2].wait_recv()
            rotate(other)
    pair_copy_e = coef_state[2]

    with scope('last'):
        for copy in last:
            copy.wait_recv()
    for copy in sent + pair_copies_h + [pair_copy_c, pair_copy_h, pair_copy_e] + last:
        copy.wait_send()

    @pl.when(jnp.logical_not(last_y))
    def _():
        ahead.wait_send()

    @pl.when(jnp.logical_not(first_y))
    def _():
        back.wait_send()

    @pl.when(jnp.logical_not(last_x))
    def _():
        to_x.wait_send()

    assert copies.used == copy_count


def deliver(corr, ham, rot, corr_out, ham_out, rot_out, sems):
    copies = [pltpu.make_async_copy(source, target, sems.at[i]) for i, (source, target) in
              enumerate(((rot, rot_out), (corr, corr_out), (ham, ham_out)))]
    for copy in copies:
        copy.start()
    for copy in copies:
        copy.wait()


def in_hbm(array):
    return pltpu.with_memory_space_constraint(array, pltpu.HBM)


def on_device(bands, potential, eigenvectors):
    gx_size, gyz_size = lax.axis_size("gx"), lax.axis_size("gyz")
    cx, cy, cz, width = bands.shape
    rows = eigenvectors.shape[0]
    cells = cx * cy * cz
    sizes = digit_sizes(gyz_size)
    count = len(sizes)
    half = width // 2
    flat = bands.reshape(cells, width)
    ham_plan, corr_plan, coef_plan = plans_of(rows, sizes)
    copy_count = 7 + peer_count(sizes, ham_plan[0][2][0]) + len(ham_plan) - 1
    copy_count += sum(2 * len(order) for _, _, order in ham_plan + corr_plan)
    copy_count += copies_of(sizes, coef_plan) + (sizes == (2, 2, 2, 2)) - 1
    copy_count += 0 if gx_size == 2 else 2 * (gx_size // 2)
    geometry = (gx_size, gyz_size, cx, cy, cz, width, rows, sizes, copy_count)

    buffers = []
    for first, last, order in ham_plan + corr_plan:
        left = list(range(count))
        for group in order:
            many = peer_count(sizes, group)
            many = 2 * many - 1 if gx_size == 2 and group == order[-1] else many - 1
            whole = tuple(sizes[i] for i in left)
            left = [d for d in left if d not in group]
            kept = tuple(sizes[i] for i in left)
            cut, line = (last - first, half), (1, half)
            buffers += [pltpu.VMEM(whole + cut, BF16), pltpu.VMEM(whole + line, F32),
                        pltpu.VMEM((many,) + kept + cut, BF16), pltpu.VMEM((many,) + kept + line, F32),
                        pltpu.VMEM(kept + cut, F32)]

    cut_x = (cx + 1) // 2
    wide, narrow = sizes + (rows, width), sizes + (rows, half)
    others = max(gx_size // 2 - 1, 1)
    vmem, anywhere = pl.BlockSpec(memory_space=pltpu.VMEM), pl.BlockSpec(memory_space=pl.ANY)
    results = (jax.ShapeDtypeStruct((rows, width), F32), jax.ShapeDtypeStruct((rows, width), F32),
               jax.ShapeDtypeStruct((cells, width), BF16))
    computed = pl.pallas_call(
        functools.partial(kernel, geometry),
        out_shape=results,
        in_specs=[pl.BlockSpec(memory_space=pltpu.HBM)] * 4,
        out_specs=(vmem, vmem, vmem),
        scratch_shapes=[
            pltpu.VMEM((cells, width), BF16), pltpu.VMEM((cy, cx, cz), F32),
            pltpu.VMEM(wide, BF16),
            pltpu.VMEM((cells, width), F32), pltpu.VMEM((cells, width), BF16),
            pltpu.VMEM(wide, F32), pltpu.VMEM(wide, F32),
            pltpu.VMEM((cut_x, cz, width), BF16), pltpu.VMEM((cx - cut_x, cz, width), BF16),
            pltpu.VMEM((cy, cz, width), BF16),
            pltpu.VMEM((2, cut_x * cz, width), BF16), pltpu.VMEM((2, width, cut_x * cz), BF16),
            pltpu.VMEM((cx * cz, width), BF16), pltpu.VMEM(narrow, BF16), pltpu.VMEM(narrow, BF16),
            pltpu.VMEM(narrow, F32), pltpu.VMEM(narrow, F32),
            pltpu.VMEM(narrow, F32), pltpu.VMEM(narrow, F32),
            pltpu.VMEM((others, rows, half), F32), pltpu.VMEM((others, rows, half), F32),
            pltpu.SemaphoreType.DMA((copy_count,)), pltpu.SemaphoreType.DMA((copy_count,)),
            pltpu.SemaphoreType.DMA((3,)), *buffers,
        ],
        compiler_params=pltpu.CompilerParams(
            collective_id=0, has_side_effects=True, vmem_limit_bytes=52 * 1024 * 1024),
    )(bands, flat, in_hbm(jnp.transpose(potential, (1, 0, 2))), in_hbm(eigenvectors))
    corr, ham, rotated = pl.pallas_call(
        deliver, out_shape=results, in_specs=[vmem] * 3, out_specs=[anywhere] * 3,
        scratch_shapes=[pltpu.SemaphoreType.DMA((3,))],
        compiler_params=pltpu.CompilerParams(vmem_limit_bytes=8 * 1024 * 1024),
    )(*computed)
    return corr, ham, rotated.reshape(bands.shape)


def solution(mesh):
    in_specs = (P("gx", "gyz", None, None), P("gx", "gyz", None), P("gyz", None))
    out_specs = (P("gyz", None), P("gyz", None), P("gx", "gyz", None, None))
    return jax.shard_map(
        on_device, mesh=mesh, in_specs=in_specs, out_specs=out_specs, check_vma=False
    )
```

```python
import functools
import itertools
import math
import types

import jax
import jax.numpy as jnp
from jax import lax
from jax.experimental import pallas as pl
from jax.experimental.pallas import tpu as pltpu
from jax.sharding import PartitionSpec as P

MESH = pl.DeviceIdType.MESH
F32, BF16 = jnp.float32, jnp.bfloat16
scope = jax.named_scope


def digit_sizes(count):
    sizes, base = [], 2 if count <= 16 else 4
    while count > 1:
        size = base if count % base == 0 else (2 if count % 2 == 0 else count)
        sizes.append(size)
        count //= size
    return tuple(reversed(sizes)) or (1,)


def gram_t(left, right):
    return lax.dot_general(left, right, (((0,), (0,)), ((), ())), preferred_element_type=F32)


def bytes_of(ref):
    return math.prod(ref.shape) * (2 if ref.dtype == BF16 else 4)


class Group:
    def __init__(self, copies, send_sem, recv_sem, whole):
        self.copies, self.send_sem, self.recv_sem, self.whole = copies, send_sem, recv_sem, whole

    def start(self, src, dst, device_id):
        self.copies.sent[self.send_sem] += bytes_of(src)
        pltpu.make_async_remote_copy(
            src_ref=src, dst_ref=dst, send_sem=self.copies.send_sems.at[self.send_sem],
            recv_sem=self.recv_sem, device_id=device_id, device_id_type=MESH).start()

    def wait_recv(self):
        pltpu.make_async_copy(self.whole, self.whole, self.recv_sem).wait()


class Copies:
    def __init__(self, send_sems, recv_sems, measures):
        self.send_sems, self.recv_sems, self.measures = send_sems, recv_sems, measures
        self.used, self.sent = 0, [0, 0]

    def group(self, whole, kind=0):
        self.used += 1
        return Group(self, kind, self.recv_sems.at[self.used - 1], whole)

    def span(self, size, kind=0):
        measure = self.measures[kind]
        row = bytes_of(measure) // measure.shape[0]
        assert size % row == 0 and size // row <= measure.shape[0]
        return measure.at[0:size // row]

    def start(self, src, dst, device_id):
        made = self.group(dst)
        made.start(src, dst, device_id)
        return made

    def wait_sends(self):
        for kind, size in enumerate(self.sent):
            whole = self.span(size, kind)
            pltpu.make_async_copy(whole, whole, self.send_sems.at[kind]).wait()


Z, XY = (0, 1), (2, 3)


def singles(order):
    return tuple((d,) for d in order)


def plans_of(rows, sizes):
    count = len(sizes)
    if sizes == (2, 2, 2, 2) and rows % 32 == 0:
        ham = ((0, rows // 2, (XY, Z)), (rows // 2, rows, (Z, XY)))
        return ham, ((0, rows, (Z, XY)),), (Z, (3,), (2,))
    fast, slow = singles(range(count)[::-1]), singles(range(count))
    return ((0, rows, fast),), ((0, rows, slow),), slow


def peer_count(sizes, group):
    return math.prod(sizes[d] for d in group)


def copies_of(sizes, order):
    return sum(peer_count(sizes, group) - 1 for group in order)


class Stream:
    def __init__(self, context, source, final, first, last, order, buffers):
        self.context, self.source, self.final, self.order = context, source, final, order
        self.rows, self.buffers = slice(first, last), buffers
        self.left, self.phase = list(range(len(context.sizes))), 0

    def index(self, values):
        return tuple(values[d] if d in values else slice(None) for d in self.left)

    def peers(self):
        group = self.order[self.phase]
        return [self.context.peer(group, k) for k in range(peer_count(self.context.sizes, group))]

    def combos(self, fixed):
        free = [d for d in self.left if d not in fixed]
        for values in itertools.product(*(range(self.context.sizes[d]) for d in free)):
            yield {**dict(zip(free, values)), **fixed}

    def diagonal(self, values, parity):
        ctx = self.context
        block = sum(values.get(d, ctx.digits[d]) * ctx.strides[d] for d in range(len(ctx.sizes)))
        shape = (self.rows.stop - self.rows.start, ctx.half)
        row = lax.broadcasted_iota(jnp.int32, shape, 0) + (block * ctx.rows + self.rows.start)
        return row == lax.broadcasted_iota(jnp.int32, shape, 1) + parity * ctx.half

    def round(self, fixed):
        out, extra = self.buffers[self.phase][:2]
        for values in self.combos(fixed):
            at = self.index(values)
            value = self.source[at + (self.rows,) if self.phase == 0 else at]
            short = value.astype(BF16)
            out[at] = short
            rest = jnp.where(self.diagonal(values, self.context.parity), value - short.astype(F32), 0.0)
            extra[at] = jnp.sum(rest, axis=0, keepdims=True)

    def open(self):
        landing, extras = self.buffers[self.phase][2:4]
        self.flights = self.context.copies.group(landing), self.context.copies.group(extras, 1)

    def ship(self, at, slot, device):
        out, extra, landing, extras = self.buffers[self.phase][:4]
        self.flights[0].start(out.at[at], landing.at[slot], device)
        self.flights[1].start(extra.at[at], extras.at[slot], device)

    def send(self, k):
        target, values = self.peers()[k]
        self.round(values)
        self.ship(self.index(values), k - 1, (self.context.gx, target))

    def start(self):
        self.open()
        for k in range(1, len(self.peers())):
            self.send(k)

    def start_both(self):
        self.open()
        self.round({})
        peers = self.peers()
        for k, (target, values) in enumerate(peers):
            at = self.index(values)
            if k:
                self.ship(at, k - 1, (self.context.gx, target))
            self.ship(at, len(peers) - 1 + k, (self.context.partner, target))

    def land(self):
        for flight in self.flights:
            flight.wait_recv()

    def finish_both(self, columns, scale):
        self.land()
        out, extra, landing, extras = self.buffers[self.phase][:4]
        many = len(self.peers())
        at = self.index(self.peers()[0][1])
        mine = [(out[at], extra[at])] + [(landing[k], extras[k]) for k in range(many - 1)]
        across = [(landing[k], extras[k]) for k in range(many - 1, 2 * many - 1)]
        parity = self.context.parity
        for column, side, parts in zip(columns, (parity, 1 - parity), (mine, across)):
            total = sum(part.astype(F32) for part, _ in parts)
            rest = sum(rest for _, rest in parts)
            total = total + jnp.where(self.diagonal({}, side), rest, 0.0)
            self.final[self.rows, column] = total * scale
        self.phase += 1

    def finish(self):
        self.land()
        _, _, landing, extras, result = self.buffers[self.phase]
        own = self.peers()[0][1]
        for values in self.combos(own):
            at = self.index(values)
            total = self.source[at + (self.rows,) if self.phase == 0 else at]
            keep = tuple(values[d] for d in self.left if d not in own)
            rest = 0.0
            for k in range(landing.shape[0]):
                total = total + landing[(k,) + keep].astype(F32)
                rest = rest + extras[(k,) + keep]
            result[keep + (Ellipsis,)] = total + jnp.where(self.diagonal(values, self.context.parity), rest, 0.0)
        self.source = result
        self.left = [d for d in self.left if d not in own]
        self.phase += 1


def kernel(geometry, grid4, rows_in, pot_in, eig, corr_out, ham_out, rot_out, flat, pot, coef, padded, hq,
           corr, ham, halo_f, halo_b, halo_x, face, turned, ghosts, late, pair_l, pair_c, pair_h, sum_c, sum_h, gx_c, gx_h,
           span, lines, send_sems, recv_sems, local_sems, *buffers):
    gx_size, gyz_size, cx, cy, cz, bands, rows, sizes, copy_count = geometry
    ham_plan, corr_plan, coef_plan = plans_of(rows, sizes)
    count = len(sizes)
    half = bands // 2
    relayed, direct = sizes == (2, 2, 2, 2), gx_size == 2
    gx, gyz = lax.axis_index("gx"), lax.axis_index("gyz")
    parity = lax.rem(gx, 2)
    partner = gx + 1 - 2 * parity
    mine = pl.ds(pl.multiple_of(parity * half, half), half)
    other = pl.ds(pl.multiple_of((1 - parity) * half, half), half)
    strides = []
    step = gyz_size
    for size in sizes:
        step //= size
        strides.append(step)
    digits = [lax.rem(gyz // stride, size) for stride, size in zip(strides, sizes)]
    copies = Copies(send_sems, recv_sems, (span, lines))

    def peer(group, k):
        target, values = gyz, {}
        for d in reversed(group):
            digit = lax.rem(digits[d] + k % sizes[d], sizes[d])
            target = target + (digit - digits[d]) * strides[d]
            values[d] = digit
            k //= sizes[d]
        return target, values

    load_flat = pltpu.make_async_copy(rows_in, flat, local_sems.at[0])
    load_flat.start()
    own_coef = coef.at[tuple(digits) + (slice(None), mine)]
    load_coef = pltpu.make_async_copy(eig.at[:, mine], own_coef, local_sems.at[1])
    load_coef.start()
    load_pot = pltpu.make_async_copy(pot_in, pot, local_sems.at[2])
    load_pot.start()

    barrier = pltpu.get_barrier_semaphore()
    first_x, last_x, first_y, last_y = gx == 0, gx == gx_size - 1, gyz == 0, gyz == gyz_size - 1
    beside = ((first_x, (gx - 1, gyz)), (last_x, (gx + 1, gyz)), (first_y, (gx, gyz - 1)), (last_y, (gx, gyz + 1)))
    for edge, device in beside:
        @pl.when(jnp.logical_not(edge))
        def _():
            pl.semaphore_signal(barrier, inc=1, device_id=device, device_id_type=MESH)
    neighbours = sum(1 - edge.astype(jnp.int32) for edge, _ in beside)
    greeted = []
    groups = []
    for _, _, order in ham_plan + corr_plan + ((0, 0, coef_plan),):
        groups += [group for group in order if group not in groups]
    wide = [group for group in groups if not any(set(group) < set(other) for other in groups)]
    for group in wide:
        greeted += [(gx, peer(group, k)[0]) for k in range(1, peer_count(sizes, group))]
    greeted += [(lax.rem(gx + 2 * k, gx_size), gyz) for k in range(1, gx_size // 2)]
    for device in greeted:
        pl.semaphore_signal(barrier, inc=1, device_id=device, device_id_type=MESH)
    with scope("barrier"):
        pl.semaphore_wait(barrier, len(greeted) + neighbours)

    def coef_send(group, held):
        many = peer_count(sizes, group) - 1
        block = coef.at[held + (slice(None), mine)]
        made = copies.group(copies.span(many * bytes_of(block)))
        for k in range(1, many + 1):
            made.start(block, block, (gx, peer(group, k)[0]))
        return [made]

    def coef_held(groups):
        done = {d for group in groups for d in group}
        return tuple(slice(None) if d in done else digits[d] for d in range(count))

    def coef_exchange():
        block = coef.at[tuple([slice(None)] * (count + 1)) + (mine,)]
        coef_state[2] = copies.start(block, block, (partner, gyz))

    def coef_wait(flying):
        for copy in flying:
            copy.wait_recv()

    def coef_start():
        coef_state[1] = coef_send(coef_plan[0], coef_held(()))

    coef_steps = 4 if relayed else len(coef_plan)

    def coef_step():
        state, at = coef_state, coef_state[0]
        state[0] += 1
        with scope("coef_%d" % at):
            if not relayed:
                coef_wait(state[1])
                if at + 1 < len(coef_plan):
                    state[1] = coef_send(coef_plan[at + 1], coef_held(coef_plan[:at + 1]))
                else:
                    coef_exchange()
                return
            held = coef_held(coef_plan[:-2])
            if at == 0:
                coef_wait(state[1])
                state[3] = coef_send(coef_plan[-1], held)
            elif at == 1:
                state[1] = coef_send(coef_plan[-2], held)
            elif at == 2:
                coef_wait(state[1])
                d, = coef_plan[-2]
                state[3] += coef_send(coef_plan[-1], held[:d] + (1 - digits[d],) + held[d + 1:])
            else:
                coef_wait(state[3])
                coef_exchange()

    coef_state = [0, None, None, []]
    load_coef.wait()

    def halo(at, src, dst, device_id):
        return pltpu.make_async_remote_copy(
            src_ref=src, dst_ref=dst, send_sem=send_sems.at[at + 2], recv_sem=recv_sems.at[copy_count + at],
            device_id=device_id, device_id_type=MESH)

    to_x = halo(0, grid4.at[cx - 1], halo_x, (lax.rem(gx + 1, gx_size), gyz))
    cut_x = (cx + 1) // 2
    ahead = halo(1, grid4.at[:cut_x, cy - 1], halo_f, (gx, lax.rem(gyz + 1, gyz_size)))
    back = halo(2, grid4.at[cut_x:, 0], halo_b, (gx, lax.rem(gyz + gyz_size - 1, gyz_size)))

    @pl.when(jnp.logical_not(last_y))
    def _():
        ahead.start()

    @pl.when(jnp.logical_not(first_y))
    def _():
        back.start()

    @pl.when(jnp.logical_not(last_x))
    def _():
        to_x.start()

    @pl.when(first_x)
    def _():
        halo_x[...] = jnp.zeros_like(halo_x)

    @pl.when(first_y)
    def _():
        halo_f[...] = jnp.zeros_like(halo_f)

    @pl.when(last_y)
    def _():
        halo_b[...] = jnp.zeros_like(halo_b)

    coef_start()

    def block_index(block):
        index = []
        for stride in strides:
            index.append(block // stride)
            block %= stride
        return tuple(index)

    def store_rows(target, first, value):
        for j in range(value.shape[0] // rows):
            target[block_index(first // rows + j)] = value[j * rows:(j + 1) * rows]

    tile = min(bands, 256)
    with scope('load'):
        load_flat.wait()
    for first in range(0, bands, tile):
        store_rows(corr, first, gram_t(flat[:, first:first + tile], flat[...]))
    everything = tuple([slice(None)] * (count + 1))
    pair_copy_c = copies.start(corr.at[everything + (other,)], pair_c, (partner, gyz))
    load_pot.wait()

    plane = cy * cz
    cells = cx * plane
    chunk = 2 * cz if cells % (2 * cz) == 0 else cz
    for first in range(0, cells, chunk):
        padded[first:first + chunk] = flat[first:first + chunk].astype(F32)
    row = lax.broadcasted_iota(jnp.int32, (cz, cz), 0)
    column = lax.broadcasted_iota(jnp.int32, (cz, cz), 1)
    zero_row = jnp.zeros((1, bands), F32)

    def segment(x, y):
        at = x * plane + y * cz
        centre = padded[at:at + cz]
        near = jnp.concatenate([zero_row, centre[:-1]]) + jnp.concatenate([centre[1:], zero_row])
        for there, offset in ((x > 0, -plane), (x < cx - 1, plane), (y > 0, -cz), (y < cy - 1, cz)):
            if there:
                near = near + padded[at + offset:at + offset + cz]
        local = jnp.broadcast_to(pot[y, x:x + 1, :], (cz, cz))
        factor = 3.0 + jnp.sum(jnp.where(row == column, local, 0.0), axis=1, keepdims=True)
        return factor * centre - 0.5 * near

    order = list(itertools.product(range(cx), range(cy)))
    per = chunk // cz
    for first in range(0, len(order), per):
        hq[first * cz:(first + per) * cz] = jnp.concatenate(
            [segment(*xy) for xy in order[first:first + per]]).astype(BF16)

    context = types.SimpleNamespace(
        copies=copies, sizes=sizes, digits=digits, strides=strides, peer=peer, gx=gx, partner=partner,
        parity=parity, rows=rows, half=half)
    taken = iter(buffers)

    scale = 1.0 / (cells * gyz_size)

    def streams(plan, source, final):
        return [Stream(context, source, final, first, last, order, [[next(taken) for _ in range(5)] for _ in order])
                for first, last, order in plan]

    ham_streams, corr_streams = streams(ham_plan, sum_h, ham_out), streams(corr_plan, sum_c, corr_out)

    def begin(group):
        for stream in group:
            stream.start()

    def end(group):
        for stream in group:
            if stream.phase == len(stream.order):
                continue
            if direct and stream.phase == len(stream.order) - 1:
                stream.finish_both((mine, other), scale)
                continue
            stream.finish()
            if direct and stream.phase == len(stream.order) - 1:
                stream.start_both()
            elif stream.phase < len(stream.order):
                stream.start()

    with scope('pair_c'):
        pair_copy_c.wait_recv()
    sum_c[...] = corr[everything + (mine,)] + pair_c[...]
    begin(corr_streams)

    def corr_step():
        at = corr_streams[0].phase
        with scope("corr_%d" % at):
            end(corr_streams)

    for first in range(0, bands, tile):
        store_rows(ham, first, gram_t(flat[:, first:first + tile], hq[...]))

    def add_cross(target, column, value):
        for j in range(bands // rows):
            index = block_index(j) + (slice(None), column)
            target[index] = target[index] - 0.5 * value[j * rows:(j + 1) * rows]

    faces = []
    for at, (cells_x, y) in enumerate(((range(cut_x), 0), (range(cut_x, cx), cy - 1))):
        own = jnp.concatenate([flat[x * plane + y * cz:x * plane + y * cz + cz] for x in cells_x])
        face[at, 0:own.shape[0]] = own
        turned[at, :, 0:own.shape[0]] = jnp.transpose(own)
        faces.append((face.at[at, 0:own.shape[0]], turned.at[at, :, 0:own.shape[0]]))

    @pl.when(jnp.logical_not(first_x))
    def _():
        to_x.wait_recv()

    near, far = flat[0:plane], jnp.concatenate([halo_x[y] for y in range(cy)])
    for first in range(0, bands, tile):
        cut = slice(first, first + tile)
        add_cross(ham, cut, gram_t(near, far[:, cut]) + gram_t(far, near[:, cut]))

    with scope('ahead'):
        @pl.when(jnp.logical_not(first_y))
        def _():
            ahead.wait_recv()

    ghosts[0:cut_x * cz] = jnp.concatenate([halo_f[x] for x in range(cut_x)])
    forward = ghosts.at[0:cut_x * cz]
    forward_t = jnp.transpose(forward[...])
    backward = ghosts.at[cut_x * cz:cx * cz]

    def cross(at, ghost, ghost_t, column):
        near, near_t = faces[at]
        return (jnp.dot(near_t[...], ghost[:, column], preferred_element_type=F32)
                + jnp.dot(ghost_t, near[:, column], preferred_element_type=F32))

    def add(column, value):
        add_cross(ham, column, value)

    add(other, cross(0, forward, forward_t, other))
    pair_copy_h = copies.start(ham.at[everything + (other,)], pair_h, (partner, gyz))
    add(mine, cross(0, forward, forward_t, mine))

    if coef_state[0] < coef_steps:
        coef_step()
    with scope('back'):
        @pl.when(jnp.logical_not(last_y))
        def _():
            back.wait_recv()

    if coef_state[0] < coef_steps:
        coef_step()
    ghosts[cut_x * cz:cx * cz] = jnp.concatenate([halo_b[x] for x in range(cx - cut_x)])
    backward_t = jnp.transpose(backward[...])
    value = cross(1, backward, backward_t, other)
    for j in range(bands // rows):
        late[block_index(j)] = (-0.5 * value[j * rows:(j + 1) * rows]).astype(BF16)
    pieces = [(ham_streams[0], k, at) for k, at in enumerate(ham_streams[0].index(values) for _, values in ham_streams[0].peers())]
    pieces = pieces[1:] + [(stream, None, everything[:-1]) for stream in ham_streams[1:]] + pieces[:1]
    pair_copies_h = []
    for stream, k, at in pieces:
        at = at + (stream.rows,)
        pair_copies_h.append(copies.start(late.at[at], pair_l.at[at], (partner, gyz)))
    add(mine, cross(1, backward, backward_t, mine))
    with scope('pair_h'):
        ham_streams[0].open()
        pair_copy_h.wait_recv()
        for (stream, k, at), copy in zip(pieces, pair_copies_h):
            at = at + (stream.rows,)
            copy.wait_recv()
            sum_h[at] = ham[at + (mine,)] + pair_h[at] + pair_l[at].astype(F32)
            if k is None:
                stream.start()
            elif k:
                stream.send(k)

    def last_sum(group, gx_recv, final):
        total, others = group[0].source, []
        for k in range(1, gx_size // 2):
            target = (lax.rem(gx + 2 * k, gx_size), gyz)
            others.append(copies.start(total, gx_recv.at[k - 1], target))
        for copy in others:
            copy.wait_recv()
        total = total[...]
        for k in range(1, gx_size // 2):
            total = total + gx_recv[k - 1]
        final[:, mine] = total * scale
        return copies.start(final.at[:, mine], final.at[:, mine], (partner, gyz))

    part = max(size for size in range(16, 512, 16) if cells % size == 0)

    def rotate(column):
        some = coef[everything + (column,)].reshape(bands, half)
        for first in range(0, cells, part):
            rot_out[first:first + part, column] = jnp.dot(
                flat[first:first + part], some, preferred_element_type=F32).astype(BF16)

    last = []
    if relayed:
        steps = ["corr", "coef", "ham", "coef", "rot", "corr", "ham"]
    else:
        steps = ["coef"] * (coef_steps - coef_state[0]) + ["rot"]
        steps += ["corr"] * len(corr_plan[0][2]) + ["ham"] * len(ham_plan[0][2])
    for step in steps:
        if step == "corr":
            corr_step()
            if corr_streams[0].phase == len(corr_streams[0].order):
                last += [] if direct else [last_sum(corr_streams, gx_c, corr_out)]
        if step == "ham":
            at = ham_streams[0].phase
            for which, stream in enumerate(ham_streams):
                with scope("ham%d_%d" % (which, at)):
                    end([stream])
            if ham_streams[0].phase == len(ham_streams[0].order):
                last += [] if direct else [last_sum(ham_streams, gx_h, ham_out)]
        if step == "coef":
            coef_step()
        if step == "rot":
            rotate(mine)
            with scope("pair_e"):
                coef_state[2].wait_recv()
            rotate(other)
    with scope('last'):
        for copy in last:
            copy.wait_recv()
    copies.wait_sends()

    @pl.when(jnp.logical_not(last_y))
    def _():
        ahead.wait_send()

    @pl.when(jnp.logical_not(first_y))
    def _():
        back.wait_send()

    @pl.when(jnp.logical_not(last_x))
    def _():
        to_x.wait_send()

    assert copies.used == copy_count


def deliver(corr, ham, rot, corr_out, ham_out, rot_out, sems):
    copies = [pltpu.make_async_copy(source, target, sems.at[i]) for i, (source, target) in
              enumerate(((rot, rot_out), (corr, corr_out), (ham, ham_out)))]
    for copy in copies:
        copy.start()
    for copy in copies:
        copy.wait()


def in_hbm(array):
    return pltpu.with_memory_space_constraint(array, pltpu.HBM)


def on_device(bands, potential, eigenvectors):
    gx_size, gyz_size = lax.axis_size("gx"), lax.axis_size("gyz")
    cx, cy, cz, width = bands.shape
    rows = eigenvectors.shape[0]
    cells = cx * cy * cz
    sizes = digit_sizes(gyz_size)
    count = len(sizes)
    half = width // 2
    flat = bands.reshape(cells, width)
    ham_plan, corr_plan, coef_plan = plans_of(rows, sizes)
    copy_count = 4 + peer_count(sizes, ham_plan[0][2][0]) + len(ham_plan) - 1
    copy_count += sum(2 * len(order) for _, _, order in ham_plan + corr_plan)
    copy_count += len(coef_plan) + (sizes == (2, 2, 2, 2)) - 1
    copy_count += 0 if gx_size == 2 else 2 * (gx_size // 2)
    geometry = (gx_size, gyz_size, cx, cy, cz, width, rows, sizes, copy_count)

    buffers = []
    for first, last, order in ham_plan + corr_plan:
        left = list(range(count))
        for group in order:
            many = peer_count(sizes, group)
            many = 2 * many - 1 if gx_size == 2 and group == order[-1] else many - 1
            whole = tuple(sizes[i] for i in left)
            left = [d for d in left if d not in group]
            kept = tuple(sizes[i] for i in left)
            cut, line = (last - first, half), (1, half)
            buffers += [pltpu.VMEM(whole + cut, BF16), pltpu.VMEM(whole + line, F32),
                        pltpu.VMEM((many,) + kept + cut, BF16), pltpu.VMEM((many,) + kept + line, F32),
                        pltpu.VMEM(kept + cut, F32)]

    cut_x = (cx + 1) // 2
    wide, narrow = sizes + (rows, width), sizes + (rows, half)
    others = max(gx_size // 2 - 1, 1)
    vmem, anywhere = pl.BlockSpec(memory_space=pltpu.VMEM), pl.BlockSpec(memory_space=pl.ANY)
    results = (jax.ShapeDtypeStruct((rows, width), F32), jax.ShapeDtypeStruct((rows, width), F32),
               jax.ShapeDtypeStruct((cells, width), BF16))
    computed = pl.pallas_call(
        functools.partial(kernel, geometry),
        out_shape=results,
        in_specs=[pl.BlockSpec(memory_space=pltpu.HBM)] * 4,
        out_specs=(vmem, vmem, vmem),
        scratch_shapes=[
            pltpu.VMEM((cells, width), BF16), pltpu.VMEM((cy, cx, cz), F32),
            pltpu.VMEM(wide, BF16),
            pltpu.VMEM((cells, width), F32), pltpu.VMEM((cells, width), BF16),
            pltpu.VMEM(wide, F32), pltpu.VMEM(wide, F32),
            pltpu.VMEM((cut_x, cz, width), BF16), pltpu.VMEM((cx - cut_x, cz, width), BF16),
            pltpu.VMEM((cy, cz, width), BF16),
            pltpu.VMEM((2, cut_x * cz, width), BF16), pltpu.VMEM((2, width, cut_x * cz), BF16),
            pltpu.VMEM((cx * cz, width), BF16), pltpu.VMEM(narrow, BF16), pltpu.VMEM(narrow, BF16),
            pltpu.VMEM(narrow, F32), pltpu.VMEM(narrow, F32),
            pltpu.VMEM(narrow, F32), pltpu.VMEM(narrow, F32),
            pltpu.VMEM((others, rows, half), F32), pltpu.VMEM((others, rows, half), F32),
            pltpu.VMEM((cells * width // 1024, 8, 128), F32), pltpu.VMEM((256, 1, half), F32),
            pltpu.SemaphoreType.DMA((5,)), pltpu.SemaphoreType.DMA((copy_count + 3,)),
            pltpu.SemaphoreType.DMA((3,)), *buffers,
        ],
        compiler_params=pltpu.CompilerParams(
            collective_id=0, has_side_effects=True, vmem_limit_bytes=52 * 1024 * 1024),
    )(bands, flat, in_hbm(jnp.transpose(potential, (1, 0, 2))), in_hbm(eigenvectors))
    corr, ham, rotated = pl.pallas_call(
        deliver, out_shape=results, in_specs=[vmem] * 3, out_specs=[anywhere] * 3,
        scratch_shapes=[pltpu.SemaphoreType.DMA((3,))],
        compiler_params=pltpu.CompilerParams(vmem_limit_bytes=8 * 1024 * 1024),
    )(*computed)
    return corr, ham, rotated.reshape(bands.shape)


def solution(mesh):
    in_specs = (P("gx", "gyz", None, None), P("gx", "gyz", None), P("gyz", None))
    out_specs = (P("gyz", None), P("gyz", None), P("gx", "gyz", None, None))
    return jax.shard_map(
        on_device, mesh=mesh, in_specs=in_specs, out_specs=out_specs, check_vma=False
    )
```

```python
import functools
import itertools
import math
import types

import jax
import jax.numpy as jnp
from jax import lax
from jax.experimental import pallas as pl
from jax.experimental.pallas import tpu as pltpu
from jax.sharding import PartitionSpec as P

MESH = pl.DeviceIdType.MESH
F32, BF16 = jnp.float32, jnp.bfloat16
scope = jax.named_scope


def digit_sizes(count):
    sizes, base = [], 2 if count <= 16 else 4
    while count > 1:
        size = base if count % base == 0 else (2 if count % 2 == 0 else count)
        sizes.append(size)
        count //= size
    return tuple(reversed(sizes)) or (1,)


def gram_t(left, right):
    return lax.dot_general(left, right, (((0,), (0,)), ((), ())), preferred_element_type=F32)


def bytes_of(ref):
    return math.prod(ref.shape) * (2 if ref.dtype == BF16 else 4)


class Group:
    def __init__(self, copies, send_sem, recv_sem, whole):
        self.copies, self.send_sem, self.recv_sem, self.whole = copies, send_sem, recv_sem, whole

    def start(self, src, dst, device_id):
        self.copies.sent[self.send_sem] += bytes_of(src)
        pltpu.make_async_remote_copy(
            src_ref=src, dst_ref=dst, send_sem=self.copies.send_sems.at[self.send_sem],
            recv_sem=self.recv_sem, device_id=device_id, device_id_type=MESH).start()

    def wait_recv(self):
        pltpu.make_async_copy(self.whole, self.whole, self.recv_sem).wait()


class Copies:
    def __init__(self, send_sems, recv_sems, measures):
        self.send_sems, self.recv_sems, self.measures = send_sems, recv_sems, measures
        self.used, self.sent = 0, [0, 0]

    def group(self, whole, kind=0):
        self.used += 1
        return Group(self, kind, self.recv_sems.at[self.used - 1], whole)

    def span(self, size, kind=0):
        measure = self.measures[kind]
        row = bytes_of(measure) // measure.shape[0]
        assert size % row == 0 and size // row <= measure.shape[0]
        return measure.at[0:size // row]

    def start(self, src, dst, device_id):
        made = self.group(dst)
        made.start(src, dst, device_id)
        return made

    def wait_sends(self):
        for kind, size in enumerate(self.sent):
            whole = self.span(size, kind)
            pltpu.make_async_copy(whole, whole, self.send_sems.at[kind]).wait()


Z, XY = (0, 1), (2, 3)


def singles(order):
    return tuple((d,) for d in order)


def plans_of(rows, sizes):
    count = len(sizes)
    if sizes == (2, 2, 2, 2) and rows % 32 == 0:
        ham = ((0, rows // 2, (XY, Z)), (rows // 2, rows, (Z, XY)))
        return ham, ((0, rows, (Z, XY)),), (Z, (3,), (2,))
    fast, slow = singles(range(count)[::-1]), singles(range(count))
    return ((0, rows, fast),), ((0, rows, slow),), slow


def peer_count(sizes, group):
    return math.prod(sizes[d] for d in group)


def copies_of(sizes, order):
    return sum(peer_count(sizes, group) - 1 for group in order)


class Stream:
    def __init__(self, context, source, final, both, first, last, order, buffers):
        self.context, self.source, self.final, self.order = context, source, final, order
        self.rows, self.buffers, self.both = slice(first, last), buffers, both
        self.left, self.phase = list(range(len(context.sizes))), 0

    def index(self, values):
        return tuple(values[d] if d in values else slice(None) for d in self.left)

    def peers(self):
        group = self.order[self.phase]
        return [self.context.peer(group, k) for k in range(peer_count(self.context.sizes, group))]

    def combos(self, fixed):
        free = [d for d in self.left if d not in fixed]
        for values in itertools.product(*(range(self.context.sizes[d]) for d in free)):
            yield {**dict(zip(free, values)), **fixed}

    def diagonal(self, values, parity):
        ctx = self.context
        block = sum(values.get(d, ctx.digits[d]) * ctx.strides[d] for d in range(len(ctx.sizes)))
        shape = (self.rows.stop - self.rows.start, ctx.half)
        row = lax.broadcasted_iota(jnp.int32, shape, 0) + (block * ctx.rows + self.rows.start)
        return row == lax.broadcasted_iota(jnp.int32, shape, 1) + parity * ctx.half

    def place(self, values):
        group = self.order[self.phase]
        line = 0
        for d in self.left:
            if d not in group and d in values:
                line = line * self.context.sizes[d] + values[d]
        return tuple(values[d] for d in self.left if d in group), slice(line, line + 1)

    def round(self, fixed):
        out, extra = self.buffers[self.phase][:2]
        for values in self.combos(fixed):
            at = self.index(values)
            value = self.source[at + (self.rows,) if self.phase == 0 else at]
            short = value.astype(BF16)
            out[at] = short
            rest = jnp.where(self.diagonal(values, self.context.parity), value - short.astype(F32), 0.0)
            spot, line = self.place(values)
            extra[spot + (line,)] = jnp.sum(rest, axis=0, keepdims=True)

    def open(self):
        landing, extras = self.buffers[self.phase][2:4]
        self.flights = self.context.copies.group(landing), self.context.copies.group(extras, 1)

    def ship(self, values, slot, device):
        out, extra, landing, extras = self.buffers[self.phase][:4]
        self.flights[0].start(out.at[self.index(values)], landing.at[slot], device)
        self.flights[1].start(extra.at[self.place(values)[0]], extras.at[slot], device)

    def send(self, k):
        target, values = self.peers()[k]
        self.round(values)
        self.ship(values, k - 1, (self.context.gx, target))

    def start(self):
        self.open()
        for k in range(1, len(self.peers())):
            self.send(k)

    def start_both(self):
        self.open()
        self.round({})
        peers = self.peers()
        for k, (target, values) in enumerate(peers):
            if k:
                self.ship(values, k - 1, (self.context.gx, target))
            self.ship(values, len(peers) - 1 + k, (self.context.partner, target))

    def land(self):
        for flight in self.flights:
            flight.wait_recv()

    def finish_both(self, columns, scale):
        self.land()
        out, extra, landing, extras = self.buffers[self.phase][:4]
        many = len(self.peers())
        at = self.index(self.peers()[0][1])
        own = extra[self.place(self.peers()[0][1])[0]]
        mine = [(out[at], own)] + [(landing[k], extras[k]) for k in range(many - 1)]
        across = [(landing[k], extras[k]) for k in range(many - 1, 2 * many - 1)]
        parity = self.context.parity
        for column, side, parts in zip(columns, (parity, 1 - parity), (mine, across)):
            total = sum(part.astype(F32) for part, _ in parts)
            rest = sum(rest for _, rest in parts)
            total = total + jnp.where(self.diagonal({}, side), rest, 0.0)
            self.final[self.rows, column] = total * scale
        self.phase += 1

    def finish(self):
        self.land()
        _, _, landing, extras, result = self.buffers[self.phase]
        own = self.peers()[0][1]
        for values in self.combos(own):
            at = self.index(values)
            total = self.source[at + (self.rows,) if self.phase == 0 else at]
            keep = tuple(values[d] for d in self.left if d not in own)
            rest = 0.0
            for k in range(landing.shape[0]):
                total = total + landing[(k,) + keep].astype(F32)
                rest = rest + extras[k, self.place(values)[1]]
            result[keep + (Ellipsis,)] = total + jnp.where(self.diagonal(values, self.context.parity), rest, 0.0)
        self.source = result
        self.left = [d for d in self.left if d not in own]
        self.phase += 1


def kernel(geometry, grid4, rows_in, pot_in, eig, corr_out, ham_out, rot_out, flat, pot, coef, padded, hq,
           corr, ham, halo_f, halo_b, halo_x, face, turned, ghosts, late, pair_l, pair_c, pair_h, sum_c, sum_h, gx_c, gx_h,
           span, lines, send_sems, recv_sems, local_sems, *buffers):
    gx_size, gyz_size, cx, cy, cz, bands, rows, sizes, copy_count = geometry
    ham_plan, corr_plan, coef_plan = plans_of(rows, sizes)
    count = len(sizes)
    half = bands // 2
    relayed, direct = sizes == (2, 2, 2, 2), gx_size == 2
    gx, gyz = lax.axis_index("gx"), lax.axis_index("gyz")
    parity = lax.rem(gx, 2)
    partner = gx + 1 - 2 * parity
    mine = pl.ds(pl.multiple_of(parity * half, half), half)
    other = pl.ds(pl.multiple_of((1 - parity) * half, half), half)
    strides = []
    step = gyz_size
    for size in sizes:
        step //= size
        strides.append(step)
    digits = [lax.rem(gyz // stride, size) for stride, size in zip(strides, sizes)]
    copies = Copies(send_sems, recv_sems, (span, lines))

    def peer(group, k):
        target, values = gyz, {}
        for d in reversed(group):
            digit = lax.rem(digits[d] + k % sizes[d], sizes[d])
            target = target + (digit - digits[d]) * strides[d]
            values[d] = digit
            k //= sizes[d]
        return target, values

    load_flat = pltpu.make_async_copy(rows_in, flat, local_sems.at[0])
    load_flat.start()
    own_coef = coef.at[tuple(digits) + (slice(None), mine)]
    load_coef = pltpu.make_async_copy(eig.at[:, mine], own_coef, local_sems.at[1])
    load_coef.start()
    load_pot = pltpu.make_async_copy(pot_in, pot, local_sems.at[2])
    load_pot.start()

    barrier = pltpu.get_barrier_semaphore()
    first_x, last_x, first_y, last_y = gx == 0, gx == gx_size - 1, gyz == 0, gyz == gyz_size - 1
    beside = ((first_x, (gx - 1, gyz)), (last_x, (gx + 1, gyz)), (first_y, (gx, gyz - 1)), (last_y, (gx, gyz + 1)))
    for edge, device in beside:
        @pl.when(jnp.logical_not(edge))
        def _():
            pl.semaphore_signal(barrier, inc=1, device_id=device, device_id_type=MESH)
    neighbours = sum(1 - edge.astype(jnp.int32) for edge, _ in beside)
    greeted = []
    groups = []
    for _, _, order in ham_plan + corr_plan + ((0, 0, coef_plan),):
        groups += [group for group in order if group not in groups]
    wide = [group for group in groups if not any(set(group) < set(other) for other in groups)]
    for group in wide:
        greeted += [(gx, peer(group, k)[0]) for k in range(1, peer_count(sizes, group))]
    greeted += [(lax.rem(gx + 2 * k, gx_size), gyz) for k in range(1, gx_size // 2)]
    for device in greeted:
        pl.semaphore_signal(barrier, inc=1, device_id=device, device_id_type=MESH)
    with scope("barrier"):
        pl.semaphore_wait(barrier, len(greeted) + neighbours)

    def coef_send(group, held):
        many = peer_count(sizes, group) - 1
        block = coef.at[held + (slice(None), mine)]
        made = copies.group(copies.span(many * bytes_of(block)))
        for k in range(1, many + 1):
            made.start(block, block, (gx, peer(group, k)[0]))
        return [made]

    def coef_held(groups):
        done = {d for group in groups for d in group}
        return tuple(slice(None) if d in done else digits[d] for d in range(count))

    def coef_exchange():
        block = coef.at[tuple([slice(None)] * (count + 1)) + (mine,)]
        coef_state[2] = copies.start(block, block, (partner, gyz))

    def coef_wait(flying):
        for copy in flying:
            copy.wait_recv()

    def coef_start():
        coef_state[1] = coef_send(coef_plan[0], coef_held(()))

    coef_steps = 4 if relayed else len(coef_plan)

    def coef_step():
        state, at = coef_state, coef_state[0]
        state[0] += 1
        with scope("coef_%d" % at):
            if not relayed:
                coef_wait(state[1])
                if at + 1 < len(coef_plan):
                    state[1] = coef_send(coef_plan[at + 1], coef_held(coef_plan[:at + 1]))
                else:
                    coef_exchange()
                return
            held = coef_held(coef_plan[:-2])
            if at == 0:
                coef_wait(state[1])
                state[3] = coef_send(coef_plan[-1], held)
            elif at == 1:
                state[1] = coef_send(coef_plan[-2], held)
            elif at == 2:
                y, x = coef_plan[-1][0], coef_plan[-2][0]
                coef_wait(state[1])
                across = held[:x] + (1 - digits[x],) + held[x + 1:]
                relayed_y = coef_send((y,), (0,) + across[1:])
                coef_wait(state[3])
                across = held[:y] + (1 - digits[y],) + held[y + 1:]
                state[3] = relayed_y + coef_send((x,), (1,) + across[1:])
            else:
                coef_wait(state[3])
                coef_exchange()

    coef_state = [0, None, None, []]
    load_coef.wait()

    def halo(at, src, dst, device_id):
        return pltpu.make_async_remote_copy(
            src_ref=src, dst_ref=dst, send_sem=send_sems.at[at + 2], recv_sem=recv_sems.at[copy_count + at],
            device_id=device_id, device_id_type=MESH)

    to_x = halo(0, grid4.at[cx - 1], halo_x, (lax.rem(gx + 1, gx_size), gyz))
    cut_x = (cx + 1) // 2
    ahead = halo(1, grid4.at[:cut_x, cy - 1], halo_f, (gx, lax.rem(gyz + 1, gyz_size)))
    back = halo(2, grid4.at[cut_x:, 0], halo_b, (gx, lax.rem(gyz + gyz_size - 1, gyz_size)))

    @pl.when(jnp.logical_not(last_y))
    def _():
        ahead.start()

    @pl.when(jnp.logical_not(first_y))
    def _():
        back.start()

    @pl.when(jnp.logical_not(last_x))
    def _():
        to_x.start()

    @pl.when(first_x)
    def _():
        halo_x[...] = jnp.zeros_like(halo_x)

    @pl.when(first_y)
    def _():
        halo_f[...] = jnp.zeros_like(halo_f)

    @pl.when(last_y)
    def _():
        halo_b[...] = jnp.zeros_like(halo_b)

    coef_start()

    def block_index(block):
        index = []
        for stride in strides:
            index.append(block // stride)
            block %= stride
        return tuple(index)

    def store_rows(target, first, value):
        for j in range(value.shape[0] // rows):
            target[block_index(first // rows + j)] = value[j * rows:(j + 1) * rows]

    tile = min(bands, 256)
    with scope('load'):
        load_flat.wait()
    for first in range(0, bands, tile):
        store_rows(corr, first, gram_t(flat[:, first:first + tile], flat[...]))
    everything = tuple([slice(None)] * (count + 1))
    pair_copy_c = copies.start(corr.at[everything + (other,)], pair_c, (partner, gyz))
    load_pot.wait()

    plane = cy * cz
    cells = cx * plane
    chunk = 2 * cz if cells % (2 * cz) == 0 else cz
    for first in range(0, cells, chunk):
        padded[first:first + chunk] = flat[first:first + chunk].astype(F32)
    row = lax.broadcasted_iota(jnp.int32, (cz, cz), 0)
    column = lax.broadcasted_iota(jnp.int32, (cz, cz), 1)
    zero_row = jnp.zeros((1, bands), F32)

    def segment(x, y):
        at = x * plane + y * cz
        centre = padded[at:at + cz]
        near = jnp.concatenate([zero_row, centre[:-1]]) + jnp.concatenate([centre[1:], zero_row])
        for there, offset in ((x > 0, -plane), (x < cx - 1, plane), (y > 0, -cz), (y < cy - 1, cz)):
            if there:
                near = near + padded[at + offset:at + offset + cz]
        local = jnp.broadcast_to(pot[y, x:x + 1, :], (cz, cz))
        factor = 3.0 + jnp.sum(jnp.where(row == column, local, 0.0), axis=1, keepdims=True)
        return factor * centre - 0.5 * near

    order = list(itertools.product(range(cx), range(cy)))
    per = chunk // cz
    for first in range(0, len(order), per):
        hq[first * cz:(first + per) * cz] = jnp.concatenate(
            [segment(*xy) for xy in order[first:first + per]]).astype(BF16)

    context = types.SimpleNamespace(
        copies=copies, sizes=sizes, digits=digits, strides=strides, peer=peer, gx=gx, partner=partner,
        parity=parity, rows=rows, half=half)
    taken = iter(buffers)

    scale = 1.0 / (cells * gyz_size)

    def streams(plan, source, final, both):
        return [Stream(context, source, final, both, first, last, order, [[next(taken) for _ in range(5)] for _ in order])
                for first, last, order in plan]

    ham_streams, corr_streams = streams(ham_plan, sum_h, ham_out, direct), streams(corr_plan, sum_c, corr_out, False)

    def begin(group):
        for stream in group:
            stream.start()

    def end(group):
        for stream in group:
            if stream.phase == len(stream.order):
                continue
            if stream.both and stream.phase == len(stream.order) - 1:
                stream.finish_both((mine, other), scale)
                continue
            stream.finish()
            if stream.both and stream.phase == len(stream.order) - 1:
                stream.start_both()
            elif stream.phase < len(stream.order):
                stream.start()

    with scope('pair_c'):
        pair_copy_c.wait_recv()
    sum_c[...] = corr[everything + (mine,)] + pair_c[...]
    begin(corr_streams)

    def corr_step():
        at = corr_streams[0].phase
        with scope("corr_%d" % at):
            end(corr_streams)

    for first in range(0, bands, tile):
        store_rows(ham, first, gram_t(flat[:, first:first + tile], hq[...]))

    def add_cross(target, column, value):
        for j in range(bands // rows):
            index = block_index(j) + (slice(None), column)
            target[index] = target[index] - 0.5 * value[j * rows:(j + 1) * rows]

    faces = []
    for at, (cells_x, y) in enumerate(((range(cut_x), 0), (range(cut_x, cx), cy - 1))):
        own = jnp.concatenate([flat[x * plane + y * cz:x * plane + y * cz + cz] for x in cells_x])
        face[at, 0:own.shape[0]] = own
        turned[at, :, 0:own.shape[0]] = jnp.transpose(own)
        faces.append((face.at[at, 0:own.shape[0]], turned.at[at, :, 0:own.shape[0]]))

    @pl.when(jnp.logical_not(first_x))
    def _():
        to_x.wait_recv()

    near, far = flat[0:plane], jnp.concatenate([halo_x[y] for y in range(cy)])
    for first in range(0, bands, tile):
        cut = slice(first, first + tile)
        add_cross(ham, cut, gram_t(near, far[:, cut]) + gram_t(far, near[:, cut]))

    with scope('ahead'):
        @pl.when(jnp.logical_not(first_y))
        def _():
            ahead.wait_recv()

    ghosts[0:cut_x * cz] = jnp.concatenate([halo_f[x] for x in range(cut_x)])
    forward = ghosts.at[0:cut_x * cz]
    forward_t = jnp.transpose(forward[...])
    backward = ghosts.at[cut_x * cz:cx * cz]

    def cross(at, ghost, ghost_t, column):
        near, near_t = faces[at]
        return (jnp.dot(near_t[...], ghost[:, column], preferred_element_type=F32)
                + jnp.dot(ghost_t, near[:, column], preferred_element_type=F32))

    def add(column, value):
        add_cross(ham, column, value)

    add(other, cross(0, forward, forward_t, other))
    pair_copy_h = copies.start(ham.at[everything + (other,)], pair_h, (partner, gyz))
    add(mine, cross(0, forward, forward_t, mine))

    if coef_state[0] < coef_steps:
        coef_step()
    with scope('back'):
        @pl.when(jnp.logical_not(last_y))
        def _():
            back.wait_recv()

    if coef_state[0] < coef_steps:
        coef_step()
    ghosts[cut_x * cz:cx * cz] = jnp.concatenate([halo_b[x] for x in range(cx - cut_x)])
    backward_t = jnp.transpose(backward[...])
    value = cross(1, backward, backward_t, other)
    for j in range(bands // rows):
        late[block_index(j)] = (-0.5 * value[j * rows:(j + 1) * rows]).astype(BF16)
    pieces = [(ham_streams[0], k, at) for k, at in enumerate(ham_streams[0].index(values) for _, values in ham_streams[0].peers())]
    pieces = pieces[1:] + [(stream, None, everything[:-1]) for stream in ham_streams[1:]] + pieces[:1]
    pair_copies_h = []
    for stream, k, at in pieces:
        at = at + (stream.rows,)
        pair_copies_h.append(copies.start(late.at[at], pair_l.at[at], (partner, gyz)))
    add(mine, cross(1, backward, backward_t, mine))
    with scope('pair_h'):
        ham_streams[0].open()
        pair_copy_h.wait_recv()
        for (stream, k, at), copy in zip(pieces, pair_copies_h):
            at = at + (stream.rows,)
            copy.wait_recv()
            sum_h[at] = ham[at + (mine,)] + pair_h[at] + pair_l[at].astype(F32)
            if k is None:
                stream.start()
            elif k:
                stream.send(k)

    def last_sum(group, gx_recv, final):
        total, others = group[0].source, []
        for k in range(1, gx_size // 2):
            target = (lax.rem(gx + 2 * k, gx_size), gyz)
            others.append(copies.start(total, gx_recv.at[k - 1], target))
        for copy in others:
            copy.wait_recv()
        total = total[...]
        for k in range(1, gx_size // 2):
            total = total + gx_recv[k - 1]
        final[:, mine] = total * scale
        return copies.start(final.at[:, mine], final.at[:, mine], (partner, gyz))

    part = max(size for size in range(16, 512, 16) if cells % size == 0)

    def rotate(column):
        some = coef[everything + (column,)].reshape(bands, half)
        for first in range(0, cells, part):
            rot_out[first:first + part, column] = jnp.dot(
                flat[first:first + part], some, preferred_element_type=F32).astype(BF16)

    last = []
    if relayed:
        steps = ["coef", "corr", "ham", "coef", "corr", "rot", "ham"]
    else:
        steps = ["coef"] * (coef_steps - coef_state[0]) + ["rot"]
        steps += ["corr"] * len(corr_plan[0][2]) + ["ham"] * len(ham_plan[0][2])
    for step in steps:
        if step == "corr":
            corr_step()
            if corr_streams[0].phase == len(corr_streams[0].order):
                last += [last_sum(corr_streams, gx_c, corr_out)]
        if step == "ham":
            at = ham_streams[0].phase
            for which, stream in enumerate(ham_streams):
                with scope("ham%d_%d" % (which, at)):
                    end([stream])
            if ham_streams[0].phase == len(ham_streams[0].order):
                last += [] if direct else [last_sum(ham_streams, gx_h, ham_out)]
        if step == "coef":
            coef_step()
        if step == "rot":
            rotate(mine)
            with scope("pair_e"):
                coef_state[2].wait_recv()
            rotate(other)
    with scope('last'):
        for copy in last:
            copy.wait_recv()
    copies.wait_sends()

    @pl.when(jnp.logical_not(last_y))
    def _():
        ahead.wait_send()

    @pl.when(jnp.logical_not(first_y))
    def _():
        back.wait_send()

    @pl.when(jnp.logical_not(last_x))
    def _():
        to_x.wait_send()

    assert copies.used == copy_count


def deliver(corr, ham, rot, corr_out, ham_out, rot_out, sems):
    copies = [pltpu.make_async_copy(source, target, sems.at[i]) for i, (source, target) in
              enumerate(((rot, rot_out), (corr, corr_out), (ham, ham_out)))]
    for copy in copies:
        copy.start()
    for copy in copies:
        copy.wait()


def in_hbm(array):
    return pltpu.with_memory_space_constraint(array, pltpu.HBM)


def on_device(bands, potential, eigenvectors):
    gx_size, gyz_size = lax.axis_size("gx"), lax.axis_size("gyz")
    cx, cy, cz, width = bands.shape
    rows = eigenvectors.shape[0]
    cells = cx * cy * cz
    sizes = digit_sizes(gyz_size)
    count = len(sizes)
    half = width // 2
    flat = bands.reshape(cells, width)
    ham_plan, corr_plan, coef_plan = plans_of(rows, sizes)
    copy_count = 4 + peer_count(sizes, ham_plan[0][2][0]) + len(ham_plan) - 1
    copy_count += sum(2 * len(order) for _, _, order in ham_plan + corr_plan)
    copy_count += len(coef_plan) + 2 * (sizes == (2, 2, 2, 2)) - 1
    copy_count += 1 if gx_size == 2 else 2 * (gx_size // 2)
    geometry = (gx_size, gyz_size, cx, cy, cz, width, rows, sizes, copy_count)

    buffers = []
    for at, (first, last, order) in enumerate(ham_plan + corr_plan):
        left = list(range(count))
        for group in order:
            many = peer_count(sizes, group)
            many = 2 * many - 1 if gx_size == 2 and at < len(ham_plan) and group == order[-1] else many - 1
            whole, spots = tuple(sizes[i] for i in left), tuple(sizes[i] for i in left if i in group)
            left = [d for d in left if d not in group]
            kept = tuple(sizes[i] for i in left)
            cut, lines = (last - first, half), (math.prod(kept), half)
            buffers += [pltpu.VMEM(whole + cut, BF16), pltpu.VMEM(spots + lines, F32),
                        pltpu.VMEM((many,) + kept + cut, BF16), pltpu.VMEM((many,) + lines, F32),
                        pltpu.VMEM(kept + cut, F32)]

    cut_x = (cx + 1) // 2
    wide, narrow = sizes + (rows, width), sizes + (rows, half)
    others = max(gx_size // 2 - 1, 1)
    vmem, anywhere = pl.BlockSpec(memory_space=pltpu.VMEM), pl.BlockSpec(memory_space=pl.ANY)
    results = (jax.ShapeDtypeStruct((rows, width), F32), jax.ShapeDtypeStruct((rows, width), F32),
               jax.ShapeDtypeStruct((cells, width), BF16))
    computed = pl.pallas_call(
        functools.partial(kernel, geometry),
        out_shape=results,
        in_specs=[pl.BlockSpec(memory_space=pltpu.HBM)] * 4,
        out_specs=(vmem, vmem, vmem),
        scratch_shapes=[
            pltpu.VMEM((cells, width), BF16), pltpu.VMEM((cy, cx, cz), F32),
            pltpu.VMEM(wide, BF16),
            pltpu.VMEM((cells, width), F32), pltpu.VMEM((cells, width), BF16),
            pltpu.VMEM(wide, F32), pltpu.VMEM(wide, F32),
            pltpu.VMEM((cut_x, cz, width), BF16), pltpu.VMEM((cx - cut_x, cz, width), BF16),
            pltpu.VMEM((cy, cz, width), BF16),
            pltpu.VMEM((2, cut_x * cz, width), BF16), pltpu.VMEM((2, width, cut_x * cz), BF16),
            pltpu.VMEM((cx * cz, width), BF16), pltpu.VMEM(narrow, BF16), pltpu.VMEM(narrow, BF16),
            pltpu.VMEM(narrow, F32), pltpu.VMEM(narrow, F32),
            pltpu.VMEM(narrow, F32), pltpu.VMEM(narrow, F32),
            pltpu.VMEM((others, rows, half), F32), pltpu.VMEM((others, rows, half), F32),
            pltpu.VMEM((cells * width // 1024, 8, 128), F32), pltpu.VMEM((256, 1, half), F32),
            pltpu.SemaphoreType.DMA((5,)), pltpu.SemaphoreType.DMA((copy_count + 3,)),
            pltpu.SemaphoreType.DMA((3,)), *buffers,
        ],
        compiler_params=pltpu.CompilerParams(
            collective_id=0, has_side_effects=True, vmem_limit_bytes=52 * 1024 * 1024),
    )(bands, flat, in_hbm(jnp.transpose(potential, (1, 0, 2))), in_hbm(eigenvectors))
    corr, ham, rotated = pl.pallas_call(
        deliver, out_shape=results, in_specs=[vmem] * 3, out_specs=[anywhere] * 3,
        scratch_shapes=[pltpu.SemaphoreType.DMA((3,))],
        compiler_params=pltpu.CompilerParams(vmem_limit_bytes=8 * 1024 * 1024),
    )(*computed)
    return corr, ham, rotated.reshape(bands.shape)


def solution(mesh):
    in_specs = (P("gx", "gyz", None, None), P("gx", "gyz", None), P("gyz", None))
    out_specs = (P("gyz", None), P("gyz", None), P("gx", "gyz", None, None))
    return jax.shard_map(
        on_device, mesh=mesh, in_specs=in_specs, out_specs=out_specs, check_vma=False
    )
```

```python
import functools
import itertools
import math
import types

import jax
import jax.numpy as jnp
from jax import lax
from jax.experimental import pallas as pl
from jax.experimental.pallas import tpu as pltpu
from jax.sharding import PartitionSpec as P

MESH = pl.DeviceIdType.MESH
F32, BF16 = jnp.float32, jnp.bfloat16
scope = jax.named_scope


def digit_sizes(count):
    sizes, base = [], 2 if count <= 16 else 4
    while count > 1:
        size = base if count % base == 0 else (2 if count % 2 == 0 else count)
        sizes.append(size)
        count //= size
    return tuple(reversed(sizes)) or (1,)


def gram_t(left, right):
    return lax.dot_general(left, right, (((0,), (0,)), ((), ())), preferred_element_type=F32)


def bytes_of(ref):
    return math.prod(ref.shape) * (2 if ref.dtype == BF16 else 4)


class Group:
    def __init__(self, copies, recv_sem, whole):
        self.copies, self.recv_sem, self.whole = copies, recv_sem, whole

    def start(self, src, dst, device_id, kind=0):
        self.copies.sent[kind] += bytes_of(src)
        pltpu.make_async_remote_copy(
            src_ref=src, dst_ref=dst, send_sem=self.copies.send_sems.at[kind],
            recv_sem=self.recv_sem, device_id=device_id, device_id_type=MESH).start()

    def wait_recv(self):
        pltpu.make_async_copy(self.whole, self.whole, self.recv_sem).wait()


class Copies:
    def __init__(self, send_sems, recv_sems, measures):
        self.send_sems, self.recv_sems, self.measures = send_sems, recv_sems, measures
        self.used, self.sent = 0, [0, 0]

    def group(self, whole):
        self.used += 1
        return Group(self, self.recv_sems.at[self.used - 1], whole)

    def span(self, size, kind=0):
        measure = self.measures[kind]
        row = bytes_of(measure) // measure.shape[0]
        assert size % row == 0 and size // row <= measure.shape[0]
        return measure.at[0:size // row]

    def start(self, src, dst, device_id):
        made = self.group(dst)
        made.start(src, dst, device_id)
        return made

    def wait_sends(self):
        for kind, size in enumerate(self.sent):
            whole = self.span(size, kind)
            pltpu.make_async_copy(whole, whole, self.send_sems.at[kind]).wait()


Z, XY = (0, 1), (2, 3)


def singles(order):
    return tuple((d,) for d in order)


def plans_of(rows, sizes):
    count = len(sizes)
    if sizes == (2, 2, 2, 2) and rows % 32 == 0:
        ham = ((0, rows // 2, (XY, Z)), (rows // 2, rows, (Z, XY)))
        return ham, ((0, rows, (Z, XY)),), (Z, (3,), (2,))
    fast, slow = singles(range(count)[::-1]), singles(range(count))
    return ((0, rows, fast),), ((0, rows, slow),), slow


def peer_count(sizes, group):
    return math.prod(sizes[d] for d in group)


def copies_of(sizes, order):
    return sum(peer_count(sizes, group) - 1 for group in order)


def far_first(group, many):
    order = {Z: [2, 1, 3], XY: [3, 1, 2]}.get(group)
    return order if order and many == 4 else list(range(1, many))


class Stream:
    def __init__(self, context, source, final, both, first, last, order, buffers):
        self.context, self.source, self.final, self.order = context, source, final, order
        self.rows, self.buffers, self.both = slice(first, last), buffers, both
        self.left, self.phase = list(range(len(context.sizes))), 0

    def index(self, values):
        return tuple(values[d] if d in values else slice(None) for d in self.left)

    def peers(self):
        group = self.order[self.phase]
        return [self.context.peer(group, k) for k in range(peer_count(self.context.sizes, group))]

    def combos(self, fixed):
        free = [d for d in self.left if d not in fixed]
        for values in itertools.product(*(range(self.context.sizes[d]) for d in free)):
            yield {**dict(zip(free, values)), **fixed}

    def diagonal(self, values, parity):
        ctx = self.context
        block = sum(values.get(d, ctx.digits[d]) * ctx.strides[d] for d in range(len(ctx.sizes)))
        shape = (self.rows.stop - self.rows.start, ctx.half)
        row = lax.broadcasted_iota(jnp.int32, shape, 0) + (block * ctx.rows + self.rows.start)
        return row == lax.broadcasted_iota(jnp.int32, shape, 1) + parity * ctx.half

    def place(self, values):
        group = self.order[self.phase]
        line = 0
        for d in self.left:
            if d not in group and d in values:
                line = line * self.context.sizes[d] + values[d]
        return tuple(values[d] for d in self.left if d in group), slice(line, line + 1)

    def round(self, fixed):
        out, extra = self.buffers[self.phase][:2]
        for values in self.combos(fixed):
            at = self.index(values)
            value = self.source[at + (self.rows,) if self.phase == 0 else at]
            short = value.astype(BF16)
            out[at] = short
            rest = jnp.where(self.diagonal(values, self.context.parity), value - short.astype(F32), 0.0)
            spot, line = self.place(values)
            extra[spot + (line,)] = jnp.sum(rest, axis=0, keepdims=True)

    def open(self):
        landing, extras = self.buffers[self.phase][2:4]
        self.flight = self.context.copies.group(self.context.copies.span(bytes_of(landing) + bytes_of(extras), 1))

    def ship(self, values, slot, device):
        out, extra, landing, extras = self.buffers[self.phase][:4]
        self.flight.start(out.at[self.index(values)], landing.at[slot], device)
        self.flight.start(extra.at[self.place(values)[0]], extras.at[slot], device, 1)

    def send(self, k):
        target, values = self.peers()[k]
        self.round(values)
        self.ship(values, k - 1, (self.context.gx, target))

    def start(self):
        self.open()
        for k in far_first(self.order[self.phase], len(self.peers())):
            self.send(k)

    def start_both(self):
        self.open()
        self.round({})
        peers = self.peers()
        for k in far_first(self.order[self.phase], len(peers)) + [0]:
            target, values = peers[k]
            if k:
                self.ship(values, k - 1, (self.context.gx, target))
            self.ship(values, len(peers) - 1 + k, (self.context.partner, target))

    def land(self):
        self.flight.wait_recv()

    def finish_both(self, columns, scale):
        self.land()
        out, extra, landing, extras = self.buffers[self.phase][:4]
        many = len(self.peers())
        at = self.index(self.peers()[0][1])
        own = extra[self.place(self.peers()[0][1])[0]]
        mine = [(out[at], own)] + [(landing[k], extras[k]) for k in range(many - 1)]
        across = [(landing[k], extras[k]) for k in range(many - 1, 2 * many - 1)]
        parity = self.context.parity
        for column, side, parts in zip(columns, (parity, 1 - parity), (mine, across)):
            total = sum(part.astype(F32) for part, _ in parts)
            rest = sum(rest for _, rest in parts)
            total = total + jnp.where(self.diagonal({}, side), rest, 0.0)
            self.final[self.rows, column] = total * scale
        self.phase += 1

    def finish(self):
        self.land()
        _, _, landing, extras, result = self.buffers[self.phase]
        own = self.peers()[0][1]
        for values in self.combos(own):
            at = self.index(values)
            total = self.source[at + (self.rows,) if self.phase == 0 else at]
            keep = tuple(values[d] for d in self.left if d not in own)
            rest = 0.0
            for k in range(landing.shape[0]):
                total = total + landing[(k,) + keep].astype(F32)
                rest = rest + extras[k, self.place(values)[1]]
            result[keep + (Ellipsis,)] = total + jnp.where(self.diagonal(values, self.context.parity), rest, 0.0)
        self.source = result
        self.left = [d for d in self.left if d not in own]
        self.phase += 1


def kernel(geometry, grid4, rows_in, pot_in, eig, corr_out, ham_out, rot_out, flat, pot, coef, padded, hq,
           corr, ham, halo_f, halo_b, halo_x, face, turned, ghosts, late, pair_l, pair_c, pair_h, sum_c, sum_h, gx_c, gx_h,
           span, lines, send_sems, recv_sems, local_sems, *buffers):
    gx_size, gyz_size, cx, cy, cz, bands, rows, sizes, copy_count = geometry
    ham_plan, corr_plan, coef_plan = plans_of(rows, sizes)
    count = len(sizes)
    half = bands // 2
    relayed, direct = sizes == (2, 2, 2, 2), gx_size == 2
    gx, gyz = lax.axis_index("gx"), lax.axis_index("gyz")
    parity = lax.rem(gx, 2)
    partner = gx + 1 - 2 * parity
    mine = pl.ds(pl.multiple_of(parity * half, half), half)
    other = pl.ds(pl.multiple_of((1 - parity) * half, half), half)
    strides = []
    step = gyz_size
    for size in sizes:
        step //= size
        strides.append(step)
    digits = [lax.rem(gyz // stride, size) for stride, size in zip(strides, sizes)]
    copies = Copies(send_sems, recv_sems, (span, lines))

    def peer(group, k):
        target, values = gyz, {}
        for d in reversed(group):
            digit = lax.rem(digits[d] + k % sizes[d], sizes[d])
            target = target + (digit - digits[d]) * strides[d]
            values[d] = digit
            k //= sizes[d]
        return target, values

    load_flat = pltpu.make_async_copy(rows_in, flat, local_sems.at[0])
    load_flat.start()
    own_coef = coef.at[tuple(digits) + (slice(None), mine)]
    load_coef = pltpu.make_async_copy(eig.at[:, mine], own_coef, local_sems.at[1])
    load_coef.start()
    load_pot = pltpu.make_async_copy(pot_in, pot, local_sems.at[2])
    load_pot.start()

    barrier = pltpu.get_barrier_semaphore()
    first_x, last_x, first_y, last_y = gx == 0, gx == gx_size - 1, gyz == 0, gyz == gyz_size - 1
    beside = ((first_x, (gx - 1, gyz)), (last_x, (gx + 1, gyz)), (first_y, (gx, gyz - 1)), (last_y, (gx, gyz + 1)))
    for edge, device in beside:
        @pl.when(jnp.logical_not(edge))
        def _():
            pl.semaphore_signal(barrier, inc=1, device_id=device, device_id_type=MESH)
    neighbours = sum(1 - edge.astype(jnp.int32) for edge, _ in beside)
    greeted = []
    groups = []
    for _, _, order in ham_plan + corr_plan + ((0, 0, coef_plan),):
        groups += [group for group in order if group not in groups]
    wide = [group for group in groups if not any(set(group) < set(other) for other in groups)]
    for group in wide:
        greeted += [(gx, peer(group, k)[0]) for k in range(1, peer_count(sizes, group))]
    greeted += [(lax.rem(gx + 2 * k, gx_size), gyz) for k in range(1, gx_size // 2)]
    for device in greeted:
        pl.semaphore_signal(barrier, inc=1, device_id=device, device_id_type=MESH)
    with scope("barrier"):
        pl.semaphore_wait(barrier, len(greeted) + neighbours)

    def coef_send(group, held):
        many = peer_count(sizes, group) - 1
        block = coef.at[held + (slice(None), mine)]
        made = copies.group(copies.span(many * bytes_of(block)))
        for k in range(1, many + 1):
            made.start(block, block, (gx, peer(group, k)[0]))
        return [made]

    def coef_held(groups):
        done = {d for group in groups for d in group}
        return tuple(slice(None) if d in done else digits[d] for d in range(count))

    def coef_exchange():
        block = coef.at[tuple([slice(None)] * (count + 1)) + (mine,)]
        coef_state[2] = copies.start(block, block, (partner, gyz))

    def coef_wait(flying):
        for copy in flying:
            copy.wait_recv()

    def coef_start():
        coef_state[1] = coef_send(coef_plan[0], coef_held(()))

    coef_steps = 4 if relayed else len(coef_plan)

    def coef_step():
        state, at = coef_state, coef_state[0]
        state[0] += 1
        with scope("coef_%d" % at):
            if not relayed:
                coef_wait(state[1])
                if at + 1 < len(coef_plan):
                    state[1] = coef_send(coef_plan[at + 1], coef_held(coef_plan[:at + 1]))
                else:
                    coef_exchange()
                return
            held = coef_held(coef_plan[:-2])
            if at == 0:
                coef_wait(state[1])
                state[3] = coef_send(coef_plan[-1], held)
            elif at == 1:
                state[1] = coef_send(coef_plan[-2], held)
            elif at == 2:
                y, x = coef_plan[-1][0], coef_plan[-2][0]
                coef_wait(state[1])
                across = held[:x] + (1 - digits[x],) + held[x + 1:]
                relayed_y = coef_send((y,), (0,) + across[1:])
                coef_wait(state[3])
                across = held[:y] + (1 - digits[y],) + held[y + 1:]
                state[3] = relayed_y + coef_send((x,), (1,) + across[1:])
            else:
                coef_wait(state[3])
                coef_exchange()

    coef_state = [0, None, None, []]
    load_coef.wait()

    def halo(at, src, dst, device_id):
        return pltpu.make_async_remote_copy(
            src_ref=src, dst_ref=dst, send_sem=send_sems.at[at + 2], recv_sem=recv_sems.at[copy_count + at],
            device_id=device_id, device_id_type=MESH)

    to_x = halo(0, grid4.at[cx - 1], halo_x, (lax.rem(gx + 1, gx_size), gyz))
    cut_x = (cx + 1) // 2
    ahead = halo(1, grid4.at[:cut_x, cy - 1], halo_f, (gx, lax.rem(gyz + 1, gyz_size)))
    back = halo(2, grid4.at[cut_x:, 0], halo_b, (gx, lax.rem(gyz + gyz_size - 1, gyz_size)))

    @pl.when(jnp.logical_not(last_y))
    def _():
        ahead.start()

    @pl.when(jnp.logical_not(first_y))
    def _():
        back.start()

    @pl.when(jnp.logical_not(last_x))
    def _():
        to_x.start()

    @pl.when(first_x)
    def _():
        halo_x[...] = jnp.zeros_like(halo_x)

    @pl.when(first_y)
    def _():
        halo_f[...] = jnp.zeros_like(halo_f)

    @pl.when(last_y)
    def _():
        halo_b[...] = jnp.zeros_like(halo_b)

    coef_start()

    def block_index(block):
        index = []
        for stride in strides:
            index.append(block // stride)
            block %= stride
        return tuple(index)

    def store_rows(target, first, value):
        for j in range(value.shape[0] // rows):
            target[block_index(first // rows + j)] = value[j * rows:(j + 1) * rows]

    tile = min(bands, 256)
    with scope('load'):
        load_flat.wait()
    for first in range(0, bands, tile):
        store_rows(corr, first, gram_t(flat[:, first:first + tile], flat[...]))
    everything = tuple([slice(None)] * (count + 1))
    pair_copy_c = copies.start(corr.at[everything + (other,)], pair_c, (partner, gyz))
    load_pot.wait()

    plane = cy * cz
    cells = cx * plane
    chunk = 2 * cz if cells % (2 * cz) == 0 else cz
    for first in range(0, cells, chunk):
        padded[first:first + chunk] = flat[first:first + chunk].astype(F32)
    row = lax.broadcasted_iota(jnp.int32, (cz, cz), 0)
    column = lax.broadcasted_iota(jnp.int32, (cz, cz), 1)
    zero_row = jnp.zeros((1, bands), F32)

    def segment(x, y):
        at = x * plane + y * cz
        centre = padded[at:at + cz]
        near = jnp.concatenate([zero_row, centre[:-1]]) + jnp.concatenate([centre[1:], zero_row])
        for there, offset in ((x > 0, -plane), (x < cx - 1, plane), (y > 0, -cz), (y < cy - 1, cz)):
            if there:
                near = near + padded[at + offset:at + offset + cz]
        local = jnp.broadcast_to(pot[y, x:x + 1, :], (cz, cz))
        factor = 3.0 + jnp.sum(jnp.where(row == column, local, 0.0), axis=1, keepdims=True)
        return factor * centre - 0.5 * near

    order = list(itertools.product(range(cx), range(cy)))
    per = chunk // cz
    for first in range(0, len(order), per):
        hq[first * cz:(first + per) * cz] = jnp.concatenate(
            [segment(*xy) for xy in order[first:first + per]]).astype(BF16)

    context = types.SimpleNamespace(
        copies=copies, sizes=sizes, digits=digits, strides=strides, peer=peer, gx=gx, partner=partner,
        parity=parity, rows=rows, half=half)
    taken = iter(buffers)

    scale = 1.0 / (cells * gyz_size)

    def streams(plan, source, final, both):
        return [Stream(context, source, final, both, first, last, order, [[next(taken) for _ in range(5)] for _ in order])
                for first, last, order in plan]

    ham_streams, corr_streams = streams(ham_plan, sum_h, ham_out, direct), streams(corr_plan, sum_c, corr_out, False)

    def begin(group):
        for stream in group:
            stream.start()

    def end(group):
        for stream in group:
            if stream.phase == len(stream.order):
                continue
            if stream.both and stream.phase == len(stream.order) - 1:
                stream.finish_both((mine, other), scale)
                continue
            stream.finish()
            if stream.both and stream.phase == len(stream.order) - 1:
                stream.start_both()
            elif stream.phase < len(stream.order):
                stream.start()

    with scope('pair_c'):
        pair_copy_c.wait_recv()
    sum_c[...] = corr[everything + (mine,)] + pair_c[...]
    begin(corr_streams)

    def corr_step():
        at = corr_streams[0].phase
        with scope("corr_%d" % at):
            end(corr_streams)

    for first in range(0, bands, tile):
        store_rows(ham, first, gram_t(flat[:, first:first + tile], hq[...]))

    def add_cross(target, column, value):
        for j in range(bands // rows):
            index = block_index(j) + (slice(None), column)
            target[index] = target[index] - 0.5 * value[j * rows:(j + 1) * rows]

    faces = []
    for at, (cells_x, y) in enumerate(((range(cut_x), 0), (range(cut_x, cx), cy - 1))):
        own = jnp.concatenate([flat[x * plane + y * cz:x * plane + y * cz + cz] for x in cells_x])
        face[at, 0:own.shape[0]] = own
        turned[at, :, 0:own.shape[0]] = jnp.transpose(own)
        faces.append((face.at[at, 0:own.shape[0]], turned.at[at, :, 0:own.shape[0]]))

    @pl.when(jnp.logical_not(first_x))
    def _():
        to_x.wait_recv()

    near, far = flat[0:plane], jnp.concatenate([halo_x[y] for y in range(cy)])
    for first in range(0, bands, tile):
        cut = slice(first, first + tile)
        add_cross(ham, cut, gram_t(near, far[:, cut]) + gram_t(far, near[:, cut]))

    with scope('ahead'):
        @pl.when(jnp.logical_not(first_y))
        def _():
            ahead.wait_recv()

    ghosts[0:cut_x * cz] = jnp.concatenate([halo_f[x] for x in range(cut_x)])
    forward = ghosts.at[0:cut_x * cz]
    forward_t = jnp.transpose(forward[...])
    backward = ghosts.at[cut_x * cz:cx * cz]

    def cross(at, ghost, ghost_t, column):
        near, near_t = faces[at]
        return (jnp.dot(near_t[...], ghost[:, column], preferred_element_type=F32)
                + jnp.dot(ghost_t, near[:, column], preferred_element_type=F32))

    def add(column, value):
        add_cross(ham, column, value)

    add(other, cross(0, forward, forward_t, other))
    pair_copy_h = copies.start(ham.at[everything + (other,)], pair_h, (partner, gyz))
    add(mine, cross(0, forward, forward_t, mine))

    if coef_state[0] < coef_steps:
        coef_step()
    with scope('back'):
        @pl.when(jnp.logical_not(last_y))
        def _():
            back.wait_recv()

    if coef_state[0] < coef_steps:
        coef_step()
    ghosts[cut_x * cz:cx * cz] = jnp.concatenate([halo_b[x] for x in range(cx - cut_x)])
    backward_t = jnp.transpose(backward[...])
    value = cross(1, backward, backward_t, other)
    for j in range(bands // rows):
        late[block_index(j)] = (-0.5 * value[j * rows:(j + 1) * rows]).astype(BF16)
    pieces = [(ham_streams[0], k, at) for k, at in enumerate(ham_streams[0].index(values) for _, values in ham_streams[0].peers())]
    pieces = [(stream, None, everything[:-1]) for stream in ham_streams[1:]] + [pieces[k] for k in far_first(ham_streams[0].order[0], len(pieces))] + pieces[:1]
    pair_copies_h = []
    for stream, k, at in pieces:
        at = at + (stream.rows,)
        pair_copies_h.append(copies.start(late.at[at], pair_l.at[at], (partner, gyz)))
    add(mine, cross(1, backward, backward_t, mine))
    with scope('pair_h'):
        ham_streams[0].open()
        pair_copy_h.wait_recv()
        for (stream, k, at), copy in zip(pieces, pair_copies_h):
            at = at + (stream.rows,)
            copy.wait_recv()
            sum_h[at] = ham[at + (mine,)] + pair_h[at] + pair_l[at].astype(F32)
            if k is None:
                stream.start()
            elif k:
                stream.send(k)

    def last_sum(group, gx_recv, final):
        total, others = group[0].source, []
        for k in range(1, gx_size // 2):
            target = (lax.rem(gx + 2 * k, gx_size), gyz)
            others.append(copies.start(total, gx_recv.at[k - 1], target))
        for copy in others:
            copy.wait_recv()
        total = total[...]
        for k in range(1, gx_size // 2):
            total = total + gx_recv[k - 1]
        final[:, mine] = total * scale
        return copies.start(final.at[:, mine], final.at[:, mine], (partner, gyz))

    part = max(size for size in range(16, 512, 16) if cells % size == 0)

    def rotate(column):
        some = coef[everything + (column,)].reshape(bands, half)
        for first in range(0, cells, part):
            rot_out[first:first + part, column] = jnp.dot(
                flat[first:first + part], some, preferred_element_type=F32).astype(BF16)

    last = []
    if relayed:
        steps = ["coef", "corr", "ham", "coef", "corr", "rot", "ham"]
    else:
        steps = ["coef"] * (coef_steps - coef_state[0]) + ["rot"]
        steps += ["corr"] * len(corr_plan[0][2]) + ["ham"] * len(ham_plan[0][2])
    for step in steps:
        if step == "corr":
            corr_step()
            if corr_streams[0].phase == len(corr_streams[0].order):
                last += [last_sum(corr_streams, gx_c, corr_out)]
        if step == "ham":
            at = ham_streams[0].phase
            for which, stream in enumerate(ham_streams):
                with scope("ham%d_%d" % (which, at)):
                    end([stream])
            if ham_streams[0].phase == len(ham_streams[0].order):
                last += [] if direct else [last_sum(ham_streams, gx_h, ham_out)]
        if step == "coef":
            coef_step()
        if step == "rot":
            rotate(mine)
            with scope("pair_e"):
                coef_state[2].wait_recv()
            rotate(other)
    with scope('last'):
        for copy in last:
            copy.wait_recv()
    copies.wait_sends()

    @pl.when(jnp.logical_not(last_y))
    def _():
        ahead.wait_send()

    @pl.when(jnp.logical_not(first_y))
    def _():
        back.wait_send()

    @pl.when(jnp.logical_not(last_x))
    def _():
        to_x.wait_send()

    assert copies.used == copy_count


def deliver(corr, ham, rot, corr_out, ham_out, rot_out, sems):
    copies = [pltpu.make_async_copy(source, target, sems.at[i]) for i, (source, target) in
              enumerate(((rot, rot_out), (corr, corr_out), (ham, ham_out)))]
    for copy in copies:
        copy.start()
    for copy in copies:
        copy.wait()


def in_hbm(array):
    return pltpu.with_memory_space_constraint(array, pltpu.HBM)


def on_device(bands, potential, eigenvectors):
    gx_size, gyz_size = lax.axis_size("gx"), lax.axis_size("gyz")
    cx, cy, cz, width = bands.shape
    rows = eigenvectors.shape[0]
    cells = cx * cy * cz
    sizes = digit_sizes(gyz_size)
    count = len(sizes)
    half = width // 2
    flat = bands.reshape(cells, width)
    ham_plan, corr_plan, coef_plan = plans_of(rows, sizes)
    copy_count = 4 + peer_count(sizes, ham_plan[0][2][0]) + len(ham_plan) - 1
    copy_count += sum(len(order) for _, _, order in ham_plan + corr_plan)
    copy_count += len(coef_plan) + 2 * (sizes == (2, 2, 2, 2)) - 1
    copy_count += 1 if gx_size == 2 else 2 * (gx_size // 2)
    geometry = (gx_size, gyz_size, cx, cy, cz, width, rows, sizes, copy_count)

    buffers = []
    for at, (first, last, order) in enumerate(ham_plan + corr_plan):
        left = list(range(count))
        for group in order:
            many = peer_count(sizes, group)
            many = 2 * many - 1 if gx_size == 2 and at < len(ham_plan) and group == order[-1] else many - 1
            whole, spots = tuple(sizes[i] for i in left), tuple(sizes[i] for i in left if i in group)
            left = [d for d in left if d not in group]
            kept = tuple(sizes[i] for i in left)
            cut, lines = (last - first, half), (math.prod(kept), half)
            buffers += [pltpu.VMEM(whole + cut, BF16), pltpu.VMEM(spots + lines, F32),
                        pltpu.VMEM((many,) + kept + cut, BF16), pltpu.VMEM((many,) + lines, F32),
                        pltpu.VMEM(kept + cut, F32)]

    cut_x = (cx + 1) // 2
    wide, narrow = sizes + (rows, width), sizes + (rows, half)
    others = max(gx_size // 2 - 1, 1)
    vmem, anywhere = pl.BlockSpec(memory_space=pltpu.VMEM), pl.BlockSpec(memory_space=pl.ANY)
    results = (jax.ShapeDtypeStruct((rows, width), F32), jax.ShapeDtypeStruct((rows, width), F32),
               jax.ShapeDtypeStruct((cells, width), BF16))
    computed = pl.pallas_call(
        functools.partial(kernel, geometry),
        out_shape=results,
        in_specs=[pl.BlockSpec(memory_space=pltpu.HBM)] * 4,
        out_specs=(vmem, vmem, vmem),
        scratch_shapes=[
            pltpu.VMEM((cells, width), BF16), pltpu.VMEM((cy, cx, cz), F32),
            pltpu.VMEM(wide, BF16),
            pltpu.VMEM((cells, width), F32), pltpu.VMEM((cells, width), BF16),
            pltpu.VMEM(wide, F32), pltpu.VMEM(wide, F32),
            pltpu.VMEM((cut_x, cz, width), BF16), pltpu.VMEM((cx - cut_x, cz, width), BF16),
            pltpu.VMEM((cy, cz, width), BF16),
            pltpu.VMEM((2, cut_x * cz, width), BF16), pltpu.VMEM((2, width, cut_x * cz), BF16),
            pltpu.VMEM((cx * cz, width), BF16), pltpu.VMEM(narrow, BF16), pltpu.VMEM(narrow, BF16),
            pltpu.VMEM(narrow, F32), pltpu.VMEM(narrow, F32),
            pltpu.VMEM(narrow, F32), pltpu.VMEM(narrow, F32),
            pltpu.VMEM((others, rows, half), F32), pltpu.VMEM((others, rows, half), F32),
            pltpu.VMEM((cells * width // 1024, 8, 128), F32), pltpu.VMEM((256, 1, half), F32),
            pltpu.SemaphoreType.DMA((5,)), pltpu.SemaphoreType.DMA((copy_count + 3,)),
            pltpu.SemaphoreType.DMA((3,)), *buffers,
        ],
        compiler_params=pltpu.CompilerParams(
            collective_id=0, has_side_effects=True, vmem_limit_bytes=52 * 1024 * 1024),
    )(bands, flat, in_hbm(jnp.transpose(potential, (1, 0, 2))), in_hbm(eigenvectors))
    corr, ham, rotated = pl.pallas_call(
        deliver, out_shape=results, in_specs=[vmem] * 3, out_specs=[anywhere] * 3,
        scratch_shapes=[pltpu.SemaphoreType.DMA((3,))],
        compiler_params=pltpu.CompilerParams(vmem_limit_bytes=8 * 1024 * 1024),
    )(*computed)
    return corr, ham, rotated.reshape(bands.shape)


def solution(mesh):
    in_specs = (P("gx", "gyz", None, None), P("gx", "gyz", None), P("gyz", None))
    out_specs = (P("gyz", None), P("gyz", None), P("gx", "gyz", None, None))
    return jax.shard_map(
        on_device, mesh=mesh, in_specs=in_specs, out_specs=out_specs, check_vma=False
    )
```

```python
import functools
import itertools
import math
import types

import jax
import jax.numpy as jnp
from jax import lax
from jax.experimental import pallas as pl
from jax.experimental.pallas import tpu as pltpu
from jax.sharding import PartitionSpec as P

MESH = pl.DeviceIdType.MESH
F32, BF16 = jnp.float32, jnp.bfloat16
scope = jax.named_scope


def digit_sizes(count):
    sizes, base = [], 2 if count <= 16 else 4
    while count > 1:
        size = base if count % base == 0 else (2 if count % 2 == 0 else count)
        sizes.append(size)
        count //= size
    return tuple(reversed(sizes)) or (1,)


def gram_t(left, right):
    return lax.dot_general(left, right, (((0,), (0,)), ((), ())), preferred_element_type=F32)


def bytes_of(ref):
    return math.prod(ref.shape) * (2 if ref.dtype == BF16 else 4)


class Group:
    def __init__(self, copies, recv_sem, whole):
        self.copies, self.recv_sem, self.whole = copies, recv_sem, whole

    def start(self, src, dst, device_id, kind=0):
        self.copies.sent[kind] += bytes_of(src)
        pltpu.make_async_remote_copy(
            src_ref=src, dst_ref=dst, send_sem=self.copies.send_sems.at[kind],
            recv_sem=self.recv_sem, device_id=device_id, device_id_type=MESH).start()

    def wait_recv(self):
        pltpu.make_async_copy(self.whole, self.whole, self.recv_sem).wait()


class Copies:
    def __init__(self, send_sems, recv_sems, measures):
        self.send_sems, self.recv_sems, self.measures = send_sems, recv_sems, measures
        self.used, self.sent = 0, [0, 0]

    def group(self, whole):
        self.used += 1
        return Group(self, self.recv_sems.at[self.used - 1], whole)

    def span(self, size, kind=0):
        measure = self.measures[kind]
        row = bytes_of(measure) // measure.shape[0]
        assert size % row == 0 and size // row <= measure.shape[0]
        return measure.at[0:size // row]

    def start(self, src, dst, device_id):
        made = self.group(dst)
        made.start(src, dst, device_id)
        return made

    def wait_sends(self):
        for kind, size in enumerate(self.sent):
            whole = self.span(size, kind)
            pltpu.make_async_copy(whole, whole, self.send_sems.at[kind]).wait()


Z, XY = (0, 1), (2, 3)


def singles(order):
    return tuple((d,) for d in order)


def plans_of(rows, sizes):
    count = len(sizes)
    if sizes == (2, 2, 2, 2) and rows % 32 == 0:
        ham = ((0, rows // 2, (XY, Z)), (rows // 2, rows, (Z, XY)))
        return ham, ((0, rows, (Z, XY)),), (Z, (3,), (2,))
    fast, slow = singles(range(count)[::-1]), singles(range(count))
    return ((0, rows, fast),), ((0, rows, slow),), slow


def peer_count(sizes, group):
    return math.prod(sizes[d] for d in group)


def copies_of(sizes, order):
    return sum(peer_count(sizes, group) - 1 for group in order)


def far_first(group, many):
    order = {Z: [2, 1, 3], XY: [3, 1, 2]}.get(group)
    return order if order and many == 4 else list(range(1, many))


class Stream:
    def __init__(self, context, source, final, both, first, last, order, buffers):
        self.context, self.source, self.final, self.order = context, source, final, order
        self.rows, self.buffers, self.both = slice(first, last), buffers, both
        self.left, self.phase = list(range(len(context.sizes))), 0

    def index(self, values):
        return tuple(values[d] if d in values else slice(None) for d in self.left)

    def peers(self):
        group = self.order[self.phase]
        return [self.context.peer(group, k) for k in range(peer_count(self.context.sizes, group))]

    def combos(self, fixed):
        free = [d for d in self.left if d not in fixed]
        for values in itertools.product(*(range(self.context.sizes[d]) for d in free)):
            yield {**dict(zip(free, values)), **fixed}

    def diagonal(self, values, parity):
        ctx = self.context
        block = sum(values.get(d, ctx.digits[d]) * ctx.strides[d] for d in range(len(ctx.sizes)))
        shape = (self.rows.stop - self.rows.start, ctx.half)
        row = lax.broadcasted_iota(jnp.int32, shape, 0) + (block * ctx.rows + self.rows.start)
        return row == lax.broadcasted_iota(jnp.int32, shape, 1) + parity * ctx.half

    def place(self, values):
        group = self.order[self.phase]
        line = 0
        for d in self.left:
            if d not in group and d in values:
                line = line * self.context.sizes[d] + values[d]
        return tuple(values[d] for d in self.left if d in group), slice(line, line + 1)

    def round(self, fixed):
        out, extra = self.buffers[self.phase][:2]
        for values in self.combos(fixed):
            at = self.index(values)
            value = self.source[at + (self.rows,) if self.phase == 0 else at]
            short = value.astype(BF16)
            out[at] = short
            rest = jnp.where(self.diagonal(values, self.context.parity), value - short.astype(F32), 0.0)
            spot, line = self.place(values)
            extra[spot + (line,)] = jnp.sum(rest, axis=0, keepdims=True)

    def open(self):
        landing, extras = self.buffers[self.phase][2:4]
        self.flight = self.context.copies.group(self.context.copies.span(bytes_of(landing) + bytes_of(extras), 1))

    def ship(self, values, slot, device):
        out, extra, landing, extras = self.buffers[self.phase][:4]
        self.flight.start(out.at[self.index(values)], landing.at[slot], device)
        self.flight.start(extra.at[self.place(values)[0]], extras.at[slot], device, 1)

    def send(self, k):
        target, values = self.peers()[k]
        self.round(values)
        self.ship(values, k - 1, (self.context.gx, target))

    def start(self):
        self.open()
        for k in far_first(self.order[self.phase], len(self.peers())):
            self.send(k)

    def start_both(self):
        self.open()
        self.round({})
        peers = self.peers()
        for k in far_first(self.order[self.phase], len(peers)) + [0]:
            target, values = peers[k]
            if k:
                self.ship(values, k - 1, (self.context.gx, target))
            self.ship(values, len(peers) - 1 + k, (self.context.partner, target))

    def land(self):
        self.flight.wait_recv()

    def finish_both(self, columns, scale):
        self.land()
        out, extra, landing, extras = self.buffers[self.phase][:4]
        many = len(self.peers())
        at = self.index(self.peers()[0][1])
        own = extra[self.place(self.peers()[0][1])[0]]
        mine = [(out[at], own)] + [(landing[k], extras[k]) for k in range(many - 1)]
        across = [(landing[k], extras[k]) for k in range(many - 1, 2 * many - 1)]
        parity = self.context.parity
        for column, side, parts in zip(columns, (parity, 1 - parity), (mine, across)):
            total = sum(part.astype(F32) for part, _ in parts)
            rest = sum(rest for _, rest in parts)
            total = total + jnp.where(self.diagonal({}, side), rest, 0.0)
            self.final[self.rows, column] = total * scale
        self.phase += 1

    def finish(self):
        self.land()
        _, _, landing, extras, result = self.buffers[self.phase]
        own = self.peers()[0][1]
        for values in self.combos(own):
            at = self.index(values)
            total = self.source[at + (self.rows,) if self.phase == 0 else at]
            keep = tuple(values[d] for d in self.left if d not in own)
            rest = 0.0
            for k in range(landing.shape[0]):
                total = total + landing[(k,) + keep].astype(F32)
                rest = rest + extras[k, self.place(values)[1]]
            result[keep + (Ellipsis,)] = total + jnp.where(self.diagonal(values, self.context.parity), rest, 0.0)
        self.source = result
        self.left = [d for d in self.left if d not in own]
        self.phase += 1


def kernel(geometry, grid4, rows_in, pot_in, eig, corr_out, ham_out, rot_out, flat, pot, coef, padded, hq,
           corr, ham, halo_f, halo_b, halo_x, face, turned, ghosts, late, pair_l, pair_c, pair_h, sum_c, sum_h, gx_c, gx_h,
           span, lines, send_sems, recv_sems, local_sems, *buffers):
    gx_size, gyz_size, cx, cy, cz, bands, rows, sizes, copy_count = geometry
    ham_plan, corr_plan, coef_plan = plans_of(rows, sizes)
    count = len(sizes)
    half = bands // 2
    relayed, direct = sizes == (2, 2, 2, 2), gx_size == 2
    gx, gyz = lax.axis_index("gx"), lax.axis_index("gyz")
    parity = lax.rem(gx, 2)
    partner = gx + 1 - 2 * parity
    mine = pl.ds(pl.multiple_of(parity * half, half), half)
    other = pl.ds(pl.multiple_of((1 - parity) * half, half), half)
    strides = []
    step = gyz_size
    for size in sizes:
        step //= size
        strides.append(step)
    digits = [lax.rem(gyz // stride, size) for stride, size in zip(strides, sizes)]
    copies = Copies(send_sems, recv_sems, (span, lines))

    def peer(group, k):
        target, values = gyz, {}
        for d in reversed(group):
            digit = lax.rem(digits[d] + k % sizes[d], sizes[d])
            target = target + (digit - digits[d]) * strides[d]
            values[d] = digit
            k //= sizes[d]
        return target, values

    load_flat = pltpu.make_async_copy(rows_in, flat, local_sems.at[0])
    load_flat.start()
    own_coef = coef.at[tuple(digits) + (slice(None), mine)]
    load_coef = pltpu.make_async_copy(eig.at[:, mine], own_coef, local_sems.at[1])
    load_coef.start()
    load_pot = pltpu.make_async_copy(pot_in, pot, local_sems.at[2])
    load_pot.start()

    barrier = pltpu.get_barrier_semaphore()
    first_x, last_x, first_y, last_y = gx == 0, gx == gx_size - 1, gyz == 0, gyz == gyz_size - 1
    beside = ((first_x, (gx - 1, gyz)), (last_x, (gx + 1, gyz)), (first_y, (gx, gyz - 1)), (last_y, (gx, gyz + 1)))
    for edge, device in beside:
        @pl.when(jnp.logical_not(edge))
        def _():
            pl.semaphore_signal(barrier, inc=1, device_id=device, device_id_type=MESH)
    neighbours = sum(1 - edge.astype(jnp.int32) for edge, _ in beside)
    greeted = []
    groups = []
    for _, _, order in ham_plan + corr_plan + ((0, 0, coef_plan),):
        groups += [group for group in order if group not in groups]
    wide = [group for group in groups if not any(set(group) < set(other) for other in groups)]
    for group in wide:
        greeted += [(gx, peer(group, k)[0]) for k in range(1, peer_count(sizes, group))]
    greeted += [(lax.rem(gx + 2 * k, gx_size), gyz) for k in range(1, gx_size // 2)]
    for device in greeted:
        pl.semaphore_signal(barrier, inc=1, device_id=device, device_id_type=MESH)
    with scope("barrier"):
        pl.semaphore_wait(barrier, len(greeted) + neighbours)

    def coef_send(group, held):
        many = peer_count(sizes, group) - 1
        block = coef.at[held + (slice(None), mine)]
        made = copies.group(copies.span(many * bytes_of(block)))
        for k in range(1, many + 1):
            made.start(block, block, (gx, peer(group, k)[0]))
        return [made]

    def coef_held(groups):
        done = {d for group in groups for d in group}
        return tuple(slice(None) if d in done else digits[d] for d in range(count))

    def coef_exchange():
        block = coef.at[tuple([slice(None)] * (count + 1)) + (mine,)]
        coef_state[2] = copies.start(block, block, (partner, gyz))

    def coef_wait(flying):
        for copy in flying:
            copy.wait_recv()

    def coef_start():
        coef_state[1] = coef_send(coef_plan[0], coef_held(()))

    coef_steps = 4 if relayed else len(coef_plan)

    def coef_step():
        state, at = coef_state, coef_state[0]
        state[0] += 1
        with scope("coef_%d" % at):
            if not relayed:
                coef_wait(state[1])
                if at + 1 < len(coef_plan):
                    state[1] = coef_send(coef_plan[at + 1], coef_held(coef_plan[:at + 1]))
                else:
                    coef_exchange()
                return
            held = coef_held(coef_plan[:-2])
            if at == 0:
                coef_wait(state[1])
                state[3] = coef_send(coef_plan[-1], held)
            elif at == 1:
                state[1] = coef_send(coef_plan[-2], held)
            elif at == 2:
                y, x = coef_plan[-1][0], coef_plan[-2][0]
                coef_wait(state[1])
                across = held[:x] + (1 - digits[x],) + held[x + 1:]
                relayed_y = coef_send((y,), (0,) + across[1:])
                coef_wait(state[3])
                across = held[:y] + (1 - digits[y],) + held[y + 1:]
                state[3] = relayed_y + coef_send((x,), (1,) + across[1:])
            else:
                coef_wait(state[3])
                coef_exchange()

    coef_state = [0, None, None, []]
    load_coef.wait()

    def halo(at, src, dst, device_id):
        return pltpu.make_async_remote_copy(
            src_ref=src, dst_ref=dst, send_sem=send_sems.at[at + 2], recv_sem=recv_sems.at[copy_count + at],
            device_id=device_id, device_id_type=MESH)

    to_x = halo(0, grid4.at[cx - 1], halo_x, (lax.rem(gx + 1, gx_size), gyz))
    cut_x = (cx + 1) // 2
    ahead = halo(1, grid4.at[:cut_x, cy - 1], halo_f, (gx, lax.rem(gyz + 1, gyz_size)))
    back = halo(2, grid4.at[cut_x:, 0], halo_b, (gx, lax.rem(gyz + gyz_size - 1, gyz_size)))

    @pl.when(jnp.logical_not(last_y))
    def _():
        ahead.start()

    @pl.when(jnp.logical_not(first_y))
    def _():
        back.start()

    @pl.when(jnp.logical_not(last_x))
    def _():
        to_x.start()

    @pl.when(first_x)
    def _():
        halo_x[...] = jnp.zeros_like(halo_x)

    @pl.when(first_y)
    def _():
        halo_f[...] = jnp.zeros_like(halo_f)

    @pl.when(last_y)
    def _():
        halo_b[...] = jnp.zeros_like(halo_b)

    coef_start()

    def block_index(block):
        index = []
        for stride in strides:
            index.append(block // stride)
            block %= stride
        return tuple(index)

    def store_rows(target, first, value):
        for j in range(value.shape[0] // rows):
            target[block_index(first // rows + j)] = value[j * rows:(j + 1) * rows]

    tile = min(bands, 256)
    with scope('load'):
        load_flat.wait()
    for first in range(0, bands, tile):
        store_rows(corr, first, gram_t(flat[:, first:first + tile], flat[...]))
    everything = tuple([slice(None)] * (count + 1))
    pair_copy_c = copies.start(corr.at[everything + (other,)], pair_c, (partner, gyz))
    load_pot.wait()

    plane = cy * cz
    cells = cx * plane
    chunk = 2 * cz if cells % (2 * cz) == 0 else cz
    for first in range(0, cells, chunk):
        padded[first:first + chunk] = flat[first:first + chunk].astype(F32)
    row = lax.broadcasted_iota(jnp.int32, (cz, cz), 0)
    column = lax.broadcasted_iota(jnp.int32, (cz, cz), 1)
    zero_row = jnp.zeros((1, bands), F32)

    def segment(x, y):
        at = x * plane + y * cz
        centre = padded[at:at + cz]
        near = jnp.concatenate([zero_row, centre[:-1]]) + jnp.concatenate([centre[1:], zero_row])
        for there, offset in ((x > 0, -plane), (x < cx - 1, plane), (y > 0, -cz), (y < cy - 1, cz)):
            if there:
                near = near + padded[at + offset:at + offset + cz]
        local = jnp.broadcast_to(pot[y, x:x + 1, :], (cz, cz))
        factor = 3.0 + jnp.sum(jnp.where(row == column, local, 0.0), axis=1, keepdims=True)
        return factor * centre - 0.5 * near

    order = list(itertools.product(range(cx), range(cy)))
    per = chunk // cz
    for first in range(0, len(order), per):
        hq[first * cz:(first + per) * cz] = jnp.concatenate(
            [segment(*xy) for xy in order[first:first + per]]).astype(BF16)

    context = types.SimpleNamespace(
        copies=copies, sizes=sizes, digits=digits, strides=strides, peer=peer, gx=gx, partner=partner,
        parity=parity, rows=rows, half=half)
    taken = iter(buffers)

    scale = 1.0 / (cells * gyz_size)

    def streams(plan, source, final, both):
        return [Stream(context, source, final, both, first, last, order, [[next(taken) for _ in range(5)] for _ in order])
                for first, last, order in plan]

    ham_streams, corr_streams = streams(ham_plan, sum_h, ham_out, direct), streams(corr_plan, sum_c, corr_out, False)

    def begin(group):
        for stream in group:
            stream.start()

    def end(group):
        for stream in group:
            if stream.phase == len(stream.order):
                continue
            if stream.both and stream.phase == len(stream.order) - 1:
                stream.finish_both((mine, other), scale)
                continue
            stream.finish()
            if stream.both and stream.phase == len(stream.order) - 1:
                stream.start_both()
            elif stream.phase < len(stream.order):
                stream.start()

    with scope('pair_c'):
        pair_copy_c.wait_recv()
    sum_c[...] = corr[everything + (mine,)] + pair_c[...]
    begin(corr_streams)

    def corr_step():
        at = corr_streams[0].phase
        with scope("corr_%d" % at):
            end(corr_streams)

    for first in range(0, bands, tile):
        store_rows(ham, first, gram_t(flat[:, first:first + tile], hq[...]))

    def add_cross(target, column, value):
        for j in range(bands // rows):
            index = block_index(j) + (slice(None), column)
            target[index] = target[index] - 0.5 * value[j * rows:(j + 1) * rows]

    faces = []
    for at, (cells_x, y) in enumerate(((range(cut_x), 0), (range(cut_x, cx), cy - 1))):
        own = jnp.concatenate([flat[x * plane + y * cz:x * plane + y * cz + cz] for x in cells_x])
        face[at, 0:own.shape[0]] = own
        turned[at, :, 0:own.shape[0]] = jnp.transpose(own)
        faces.append((face.at[at, 0:own.shape[0]], turned.at[at, :, 0:own.shape[0]]))

    @pl.when(jnp.logical_not(first_x))
    def _():
        to_x.wait_recv()

    near, far = flat[0:plane], jnp.concatenate([halo_x[y] for y in range(cy)])
    for first in range(0, bands, tile):
        cut = slice(first, first + tile)
        add_cross(ham, cut, gram_t(near, far[:, cut]) + gram_t(far, near[:, cut]))

    with scope('ahead'):
        @pl.when(jnp.logical_not(first_y))
        def _():
            ahead.wait_recv()

    ghosts[0:cut_x * cz] = jnp.concatenate([halo_f[x] for x in range(cut_x)])
    forward = ghosts.at[0:cut_x * cz]
    forward_t = jnp.transpose(forward[...])
    backward = ghosts.at[cut_x * cz:cx * cz]

    def cross(at, ghost, ghost_t, column):
        near, near_t = faces[at]
        return (jnp.dot(near_t[...], ghost[:, column], preferred_element_type=F32)
                + jnp.dot(ghost_t, near[:, column], preferred_element_type=F32))

    def add(column, value):
        add_cross(ham, column, value)

    add(other, cross(0, forward, forward_t, other))
    pair_copy_h = copies.start(ham.at[everything + (other,)], pair_h, (partner, gyz))
    add(mine, cross(0, forward, forward_t, mine))

    if coef_state[0] < coef_steps:
        coef_step()
    with scope('back'):
        @pl.when(jnp.logical_not(last_y))
        def _():
            back.wait_recv()

    if coef_state[0] < coef_steps:
        coef_step()
    ghosts[cut_x * cz:cx * cz] = jnp.concatenate([halo_b[x] for x in range(cx - cut_x)])
    backward_t = jnp.transpose(backward[...])
    value = cross(1, backward, backward_t, other)
    for j in range(bands // rows):
        late[block_index(j)] = (-0.5 * value[j * rows:(j + 1) * rows]).astype(BF16)
    pieces = [(ham_streams[0], k, at) for k, at in enumerate(ham_streams[0].index(values) for _, values in ham_streams[0].peers())]
    pieces = [(stream, None, everything[:-1]) for stream in ham_streams[1:]] + [pieces[k] for k in far_first(ham_streams[0].order[0], len(pieces))] + pieces[:1]
    pair_copies_h = []
    for stream, k, at in pieces:
        at = at + (stream.rows,)
        pair_copies_h.append(copies.start(late.at[at], pair_l.at[at], (partner, gyz)))
    add(mine, cross(1, backward, backward_t, mine))
    with scope('pair_h'):
        ham_streams[0].open()
        pair_copy_h.wait_recv()
        sum_h[...] = ham[everything + (mine,)] + pair_h[...]
        for (stream, k, at), copy in zip(pieces, pair_copies_h):
            at = at + (stream.rows,)
            copy.wait_recv()
            sum_h[at] = sum_h[at] + pair_l[at].astype(F32)
            if k is None:
                stream.start()
            elif k:
                stream.send(k)

    def last_sum(group, gx_recv, final):
        total, others = group[0].source, []
        for k in range(1, gx_size // 2):
            target = (lax.rem(gx + 2 * k, gx_size), gyz)
            others.append(copies.start(total, gx_recv.at[k - 1], target))
        for copy in others:
            copy.wait_recv()
        total = total[...]
        for k in range(1, gx_size // 2):
            total = total + gx_recv[k - 1]
        final[:, mine] = total * scale
        return copies.start(final.at[:, mine], final.at[:, mine], (partner, gyz))

    part = max(size for size in range(16, 512, 16) if cells % size == 0)

    def rotate(column):
        some = coef[everything + (column,)].reshape(bands, half)
        for first in range(0, cells, part):
            rot_out[first:first + part, column] = jnp.dot(
                flat[first:first + part], some, preferred_element_type=F32).astype(BF16)

    last = []
    if relayed:
        steps = ["coef", "corr", "ham", "coef", "corr", "rot", "ham"]
    else:
        steps = ["coef"] * (coef_steps - coef_state[0]) + ["rot"]
        steps += ["corr"] * len(corr_plan[0][2]) + ["ham"] * len(ham_plan[0][2])
    for step in steps:
        if step == "corr":
            corr_step()
            if corr_streams[0].phase == len(corr_streams[0].order):
                last += [last_sum(corr_streams, gx_c, corr_out)]
        if step == "ham":
            at = ham_streams[0].phase
            for which, stream in enumerate(ham_streams):
                with scope("ham%d_%d" % (which, at)):
                    end([stream])
            if ham_streams[0].phase == len(ham_streams[0].order):
                last += [] if direct else [last_sum(ham_streams, gx_h, ham_out)]
        if step == "coef":
            coef_step()
        if step == "rot":
            rotate(mine)
            with scope("pair_e"):
                coef_state[2].wait_recv()
            rotate(other)
    with scope('last'):
        for copy in last:
            copy.wait_recv()
    copies.wait_sends()

    @pl.when(jnp.logical_not(last_y))
    def _():
        ahead.wait_send()

    @pl.when(jnp.logical_not(first_y))
    def _():
        back.wait_send()

    @pl.when(jnp.logical_not(last_x))
    def _():
        to_x.wait_send()

    assert copies.used == copy_count


def deliver(corr, ham, rot, corr_out, ham_out, rot_out, sems):
    copies = [pltpu.make_async_copy(source, target, sems.at[i]) for i, (source, target) in
              enumerate(((rot, rot_out), (corr, corr_out), (ham, ham_out)))]
    for copy in copies:
        copy.start()
    for copy in copies:
        copy.wait()


def in_hbm(array):
    return pltpu.with_memory_space_constraint(array, pltpu.HBM)


def on_device(bands, potential, eigenvectors):
    gx_size, gyz_size = lax.axis_size("gx"), lax.axis_size("gyz")
    cx, cy, cz, width = bands.shape
    rows = eigenvectors.shape[0]
    cells = cx * cy * cz
    sizes = digit_sizes(gyz_size)
    count = len(sizes)
    half = width // 2
    flat = bands.reshape(cells, width)
    ham_plan, corr_plan, coef_plan = plans_of(rows, sizes)
    copy_count = 4 + peer_count(sizes, ham_plan[0][2][0]) + len(ham_plan) - 1
    copy_count += sum(len(order) for _, _, order in ham_plan + corr_plan)
    copy_count += len(coef_plan) + 2 * (sizes == (2, 2, 2, 2)) - 1
    copy_count += 1 if gx_size == 2 else 2 * (gx_size // 2)
    geometry = (gx_size, gyz_size, cx, cy, cz, width, rows, sizes, copy_count)

    buffers = []
    for at, (first, last, order) in enumerate(ham_plan + corr_plan):
        left = list(range(count))
        for group in order:
            many = peer_count(sizes, group)
            many = 2 * many - 1 if gx_size == 2 and at < len(ham_plan) and group == order[-1] else many - 1
            whole, spots = tuple(sizes[i] for i in left), tuple(sizes[i] for i in left if i in group)
            left = [d for d in left if d not in group]
            kept = tuple(sizes[i] for i in left)
            cut, lines = (last - first, half), (math.prod(kept), half)
            buffers += [pltpu.VMEM(whole + cut, BF16), pltpu.VMEM(spots + lines, F32),
                        pltpu.VMEM((many,) + kept + cut, BF16), pltpu.VMEM((many,) + lines, F32),
                        pltpu.VMEM(kept + cut, F32)]

    cut_x = (cx + 1) // 2
    wide, narrow = sizes + (rows, width), sizes + (rows, half)
    others = max(gx_size // 2 - 1, 1)
    vmem, anywhere = pl.BlockSpec(memory_space=pltpu.VMEM), pl.BlockSpec(memory_space=pl.ANY)
    results = (jax.ShapeDtypeStruct((rows, width), F32), jax.ShapeDtypeStruct((rows, width), F32),
               jax.ShapeDtypeStruct((cells, width), BF16))
    computed = pl.pallas_call(
        functools.partial(kernel, geometry),
        out_shape=results,
        in_specs=[pl.BlockSpec(memory_space=pltpu.HBM)] * 4,
        out_specs=(vmem, vmem, vmem),
        scratch_shapes=[
            pltpu.VMEM((cells, width), BF16), pltpu.VMEM((cy, cx, cz), F32),
            pltpu.VMEM(wide, BF16),
            pltpu.VMEM((cells, width), F32), pltpu.VMEM((cells, width), BF16),
            pltpu.VMEM(wide, F32), pltpu.VMEM(wide, F32),
            pltpu.VMEM((cut_x, cz, width), BF16), pltpu.VMEM((cx - cut_x, cz, width), BF16),
            pltpu.VMEM((cy, cz, width), BF16),
            pltpu.VMEM((2, cut_x * cz, width), BF16), pltpu.VMEM((2, width, cut_x * cz), BF16),
            pltpu.VMEM((cx * cz, width), BF16), pltpu.VMEM(narrow, BF16), pltpu.VMEM(narrow, BF16),
            pltpu.VMEM(narrow, F32), pltpu.VMEM(narrow, F32),
            pltpu.VMEM(narrow, F32), pltpu.VMEM(narrow, F32),
            pltpu.VMEM((others, rows, half), F32), pltpu.VMEM((others, rows, half), F32),
            pltpu.VMEM((cells * width // 1024, 8, 128), F32), pltpu.VMEM((256, 1, half), F32),
            pltpu.SemaphoreType.DMA((5,)), pltpu.SemaphoreType.DMA((copy_count + 3,)),
            pltpu.SemaphoreType.DMA((3,)), *buffers,
        ],
        compiler_params=pltpu.CompilerParams(
            collective_id=0, has_side_effects=True, vmem_limit_bytes=52 * 1024 * 1024),
    )(bands, flat, in_hbm(jnp.transpose(potential, (1, 0, 2))), in_hbm(eigenvectors))
    corr, ham, rotated = pl.pallas_call(
        deliver, out_shape=results, in_specs=[vmem] * 3, out_specs=[anywhere] * 3,
        scratch_shapes=[pltpu.SemaphoreType.DMA((3,))],
        compiler_params=pltpu.CompilerParams(vmem_limit_bytes=8 * 1024 * 1024),
    )(*computed)
    return corr, ham, rotated.reshape(bands.shape)


def solution(mesh):
    in_specs = (P("gx", "gyz", None, None), P("gx", "gyz", None), P("gyz", None))
    out_specs = (P("gyz", None), P("gyz", None), P("gx", "gyz", None, None))
    return jax.shard_map(
        on_device, mesh=mesh, in_specs=in_specs, out_specs=out_specs, check_vma=False
    )
```

```python
import functools
import itertools
import math
import types

import jax
import jax.numpy as jnp
from jax import lax
from jax.experimental import pallas as pl
from jax.experimental.pallas import tpu as pltpu
from jax.sharding import PartitionSpec as P

MESH = pl.DeviceIdType.MESH
F32, BF16 = jnp.float32, jnp.bfloat16
scope = jax.named_scope


def digit_sizes(count):
    sizes, base = [], 2 if count <= 16 else 4
    while count > 1:
        size = base if count % base == 0 else (2 if count % 2 == 0 else count)
        sizes.append(size)
        count //= size
    return tuple(reversed(sizes)) or (1,)


def gram_t(left, right):
    return lax.dot_general(left, right, (((0,), (0,)), ((), ())), preferred_element_type=F32)


def bytes_of(ref):
    return math.prod(ref.shape) * (2 if ref.dtype == BF16 else 4)


class Group:
    def __init__(self, copies, recv_sem, whole):
        self.copies, self.recv_sem, self.whole = copies, recv_sem, whole

    def start(self, src, dst, device_id, kind=0):
        self.copies.sent[kind] += bytes_of(src)
        pltpu.make_async_remote_copy(
            src_ref=src, dst_ref=dst, send_sem=self.copies.send_sems.at[kind],
            recv_sem=self.recv_sem, device_id=device_id, device_id_type=MESH).start()

    def wait_recv(self):
        pltpu.make_async_copy(self.whole, self.whole, self.recv_sem).wait()


class Copies:
    def __init__(self, send_sems, recv_sems, measures):
        self.send_sems, self.recv_sems, self.measures = send_sems, recv_sems, measures
        self.used, self.sent = 0, [0, 0]

    def group(self, whole):
        self.used += 1
        return Group(self, self.recv_sems.at[self.used - 1], whole)

    def span(self, size, kind=0):
        measure = self.measures[kind]
        row = bytes_of(measure) // measure.shape[0]
        assert size % row == 0 and size // row <= measure.shape[0]
        return measure.at[0:size // row]

    def start(self, src, dst, device_id):
        made = self.group(dst)
        made.start(src, dst, device_id)
        return made

    def wait_sends(self):
        for kind, size in enumerate(self.sent):
            whole = self.span(size, kind)
            pltpu.make_async_copy(whole, whole, self.send_sems.at[kind]).wait()


Z, XY = (0, 1), (2, 3)


def singles(order):
    return tuple((d,) for d in order)


def plans_of(rows, sizes):
    count = len(sizes)
    if sizes == (2, 2, 2, 2) and rows % 32 == 0:
        ham = ((0, rows // 2, (XY, Z)), (rows // 2, rows, (Z, XY)))
        return ham, ((0, rows, (Z, XY)),), (Z, (3,), (2,))
    fast, slow = singles(range(count)[::-1]), singles(range(count))
    return ((0, rows, fast),), ((0, rows, slow),), slow


def peer_count(sizes, group):
    return math.prod(sizes[d] for d in group)


def copies_of(sizes, order):
    return sum(peer_count(sizes, group) - 1 for group in order)


def far_first(group, many, last=False):
    order = ({Z: [3, 2, 1], XY: [3, 1, 2]} if last else {Z: [2, 1, 3], XY: [3, 1, 2]}).get(group)
    return order if order and many == 4 else list(range(1, many))


class Stream:
    def __init__(self, context, source, final, both, first, last, order, buffers):
        self.context, self.source, self.final, self.order = context, source, final, order
        self.rows, self.buffers, self.both = slice(first, last), buffers, both
        self.left, self.phase = list(range(len(context.sizes))), 0

    def index(self, values):
        return tuple(values[d] if d in values else slice(None) for d in self.left)

    def peers(self):
        group = self.order[self.phase]
        return [self.context.peer(group, k) for k in range(peer_count(self.context.sizes, group))]

    def combos(self, fixed):
        free = [d for d in self.left if d not in fixed]
        for values in itertools.product(*(range(self.context.sizes[d]) for d in free)):
            yield {**dict(zip(free, values)), **fixed}

    def diagonal(self, values, parity):
        ctx = self.context
        block = sum(values.get(d, ctx.digits[d]) * ctx.strides[d] for d in range(len(ctx.sizes)))
        shape = (self.rows.stop - self.rows.start, ctx.half)
        row = lax.broadcasted_iota(jnp.int32, shape, 0) + (block * ctx.rows + self.rows.start)
        return row == lax.broadcasted_iota(jnp.int32, shape, 1) + parity * ctx.half

    def place(self, values):
        group = self.order[self.phase]
        line = 0
        for d in self.left:
            if d not in group and d in values:
                line = line * self.context.sizes[d] + values[d]
        return tuple(values[d] for d in self.left if d in group), slice(line, line + 1)

    def round(self, fixed):
        out, extra = self.buffers[self.phase][:2]
        for values in self.combos(fixed):
            at = self.index(values)
            value = self.source[at + (self.rows,) if self.phase == 0 else at]
            short = value.astype(BF16)
            out[at] = short
            rest = jnp.where(self.diagonal(values, self.context.parity), value - short.astype(F32), 0.0)
            spot, line = self.place(values)
            extra[spot + (line,)] = jnp.sum(rest, axis=0, keepdims=True)

    def open(self):
        landing, extras = self.buffers[self.phase][2:4]
        self.flight = self.context.copies.group(self.context.copies.span(bytes_of(landing) + bytes_of(extras), 1))

    def ship(self, values, slot, device):
        out, extra, landing, extras = self.buffers[self.phase][:4]
        self.flight.start(out.at[self.index(values)], landing.at[slot], device)
        self.flight.start(extra.at[self.place(values)[0]], extras.at[slot], device, 1)

    def send(self, k):
        target, values = self.peers()[k]
        self.round(values)
        self.ship(values, k - 1, (self.context.gx, target))

    def start(self):
        self.open()
        for k in far_first(self.order[self.phase], len(self.peers())):
            self.send(k)

    def start_both(self):
        self.open()
        self.round({})
        peers = self.peers()
        for k in far_first(self.order[self.phase], len(peers), True) + [0]:
            target, values = peers[k]
            if k:
                self.ship(values, k - 1, (self.context.gx, target))
            self.ship(values, len(peers) - 1 + k, (self.context.partner, target))

    def land(self):
        self.flight.wait_recv()

    def finish_both(self, columns, scale):
        self.land()
        out, extra, landing, extras = self.buffers[self.phase][:4]
        many = len(self.peers())
        at = self.index(self.peers()[0][1])
        own = extra[self.place(self.peers()[0][1])[0]]
        mine = [(out[at], own)] + [(landing[k], extras[k]) for k in range(many - 1)]
        across = [(landing[k], extras[k]) for k in range(many - 1, 2 * many - 1)]
        parity = self.context.parity
        for column, side, parts in zip(columns, (parity, 1 - parity), (mine, across)):
            total = sum(part.astype(F32) for part, _ in parts)
            rest = sum(rest for _, rest in parts)
            total = total + jnp.where(self.diagonal({}, side), rest, 0.0)
            self.final[self.rows, column] = total * scale
        self.phase += 1

    def finish(self):
        self.land()
        _, _, landing, extras, result = self.buffers[self.phase]
        own = self.peers()[0][1]
        for values in self.combos(own):
            at = self.index(values)
            total = self.source[at + (self.rows,) if self.phase == 0 else at]
            keep = tuple(values[d] for d in self.left if d not in own)
            rest = 0.0
            for k in range(landing.shape[0]):
                total = total + landing[(k,) + keep].astype(F32)
                rest = rest + extras[k, self.place(values)[1]]
            result[keep + (Ellipsis,)] = total + jnp.where(self.diagonal(values, self.context.parity), rest, 0.0)
        self.source = result
        self.left = [d for d in self.left if d not in own]
        self.phase += 1


def kernel(geometry, grid4, rows_in, pot_in, eig, corr_out, ham_out, rot_out, flat, pot, coef, padded, hq,
           corr, ham, halo_f, halo_b, halo_x, face, turned, ghosts, late, pair_l, pair_c, pair_h, sum_c, sum_h, gx_c, gx_h,
           span, lines, send_sems, recv_sems, local_sems, *buffers):
    gx_size, gyz_size, cx, cy, cz, bands, rows, sizes, copy_count = geometry
    ham_plan, corr_plan, coef_plan = plans_of(rows, sizes)
    count = len(sizes)
    half = bands // 2
    relayed, direct = sizes == (2, 2, 2, 2), gx_size == 2
    gx, gyz = lax.axis_index("gx"), lax.axis_index("gyz")
    parity = lax.rem(gx, 2)
    partner = gx + 1 - 2 * parity
    mine = pl.ds(pl.multiple_of(parity * half, half), half)
    other = pl.ds(pl.multiple_of((1 - parity) * half, half), half)
    strides = []
    step = gyz_size
    for size in sizes:
        step //= size
        strides.append(step)
    digits = [lax.rem(gyz // stride, size) for stride, size in zip(strides, sizes)]
    copies = Copies(send_sems, recv_sems, (span, lines))

    def peer(group, k):
        target, values = gyz, {}
        for d in reversed(group):
            digit = lax.rem(digits[d] + k % sizes[d], sizes[d])
            target = target + (digit - digits[d]) * strides[d]
            values[d] = digit
            k //= sizes[d]
        return target, values

    load_flat = pltpu.make_async_copy(rows_in, flat, local_sems.at[0])
    load_flat.start()
    own_coef = coef.at[tuple(digits) + (slice(None), mine)]
    load_coef = pltpu.make_async_copy(eig.at[:, mine], own_coef, local_sems.at[1])
    load_coef.start()
    load_pot = pltpu.make_async_copy(pot_in, pot, local_sems.at[2])
    load_pot.start()

    barrier = pltpu.get_barrier_semaphore()
    first_x, last_x, first_y, last_y = gx == 0, gx == gx_size - 1, gyz == 0, gyz == gyz_size - 1
    beside = ((first_x, (gx - 1, gyz)), (last_x, (gx + 1, gyz)), (first_y, (gx, gyz - 1)), (last_y, (gx, gyz + 1)))
    for edge, device in beside:
        @pl.when(jnp.logical_not(edge))
        def _():
            pl.semaphore_signal(barrier, inc=1, device_id=device, device_id_type=MESH)
    neighbours = sum(1 - edge.astype(jnp.int32) for edge, _ in beside)
    greeted = []
    groups = []
    for _, _, order in ham_plan + corr_plan + ((0, 0, coef_plan),):
        groups += [group for group in order if group not in groups]
    wide = [group for group in groups if not any(set(group) < set(other) for other in groups)]
    for group in wide:
        greeted += [(gx, peer(group, k)[0]) for k in range(1, peer_count(sizes, group))]
    greeted += [(lax.rem(gx + 2 * k, gx_size), gyz) for k in range(1, gx_size // 2)]
    for device in greeted:
        pl.semaphore_signal(barrier, inc=1, device_id=device, device_id_type=MESH)
    with scope("barrier"):
        pl.semaphore_wait(barrier, len(greeted) + neighbours)

    def coef_send(group, held):
        many = peer_count(sizes, group) - 1
        block = coef.at[held + (slice(None), mine)]
        made = copies.group(copies.span(many * bytes_of(block)))
        for k in range(1, many + 1):
            made.start(block, block, (gx, peer(group, k)[0]))
        return [made]

    def coef_held(groups):
        done = {d for group in groups for d in group}
        return tuple(slice(None) if d in done else digits[d] for d in range(count))

    def coef_exchange():
        block = coef.at[tuple([slice(None)] * (count + 1)) + (mine,)]
        coef_state[2] = copies.start(block, block, (partner, gyz))

    def coef_wait(flying):
        for copy in flying:
            copy.wait_recv()

    def coef_start():
        coef_state[1] = coef_send(coef_plan[0], coef_held(()))

    coef_steps = 4 if relayed else len(coef_plan)

    def coef_step():
        state, at = coef_state, coef_state[0]
        state[0] += 1
        with scope("coef_%d" % at):
            if not relayed:
                coef_wait(state[1])
                if at + 1 < len(coef_plan):
                    state[1] = coef_send(coef_plan[at + 1], coef_held(coef_plan[:at + 1]))
                else:
                    coef_exchange()
                return
            held = coef_held(coef_plan[:-2])
            if at == 0:
                coef_wait(state[1])
                state[3] = coef_send(coef_plan[-1], held)
            elif at == 1:
                state[1] = coef_send(coef_plan[-2], held)
            elif at == 2:
                y, x = coef_plan[-1][0], coef_plan[-2][0]
                coef_wait(state[1])
                across = held[:x] + (1 - digits[x],) + held[x + 1:]
                relayed_y = coef_send((y,), (0,) + across[1:])
                coef_wait(state[3])
                across = held[:y] + (1 - digits[y],) + held[y + 1:]
                state[3] = relayed_y + coef_send((x,), (1,) + across[1:])
            else:
                coef_wait(state[3])
                coef_exchange()

    coef_state = [0, None, None, []]
    load_coef.wait()

    def halo(at, src, dst, device_id):
        return pltpu.make_async_remote_copy(
            src_ref=src, dst_ref=dst, send_sem=send_sems.at[at + 2], recv_sem=recv_sems.at[copy_count + at],
            device_id=device_id, device_id_type=MESH)

    to_x = halo(0, grid4.at[cx - 1], halo_x, (lax.rem(gx + 1, gx_size), gyz))
    cut_x = (cx + 1) // 2
    ahead = halo(1, grid4.at[:cut_x, cy - 1], halo_f, (gx, lax.rem(gyz + 1, gyz_size)))
    back = halo(2, grid4.at[cut_x:, 0], halo_b, (gx, lax.rem(gyz + gyz_size - 1, gyz_size)))

    @pl.when(jnp.logical_not(last_y))
    def _():
        ahead.start()

    @pl.when(jnp.logical_not(first_y))
    def _():
        back.start()

    @pl.when(jnp.logical_not(last_x))
    def _():
        to_x.start()

    @pl.when(first_x)
    def _():
        halo_x[...] = jnp.zeros_like(halo_x)

    @pl.when(first_y)
    def _():
        halo_f[...] = jnp.zeros_like(halo_f)

    @pl.when(last_y)
    def _():
        halo_b[...] = jnp.zeros_like(halo_b)

    coef_start()

    def block_index(block):
        index = []
        for stride in strides:
            index.append(block // stride)
            block %= stride
        return tuple(index)

    def store_rows(target, first, value):
        for j in range(value.shape[0] // rows):
            target[block_index(first // rows + j)] = value[j * rows:(j + 1) * rows]

    tile = min(bands, 256)
    with scope('load'):
        load_flat.wait()
    for first in range(0, bands, tile):
        store_rows(corr, first, gram_t(flat[:, first:first + tile], flat[...]))
    everything = tuple([slice(None)] * (count + 1))
    pair_copy_c = copies.start(corr.at[everything + (other,)], pair_c, (partner, gyz))
    load_pot.wait()

    plane = cy * cz
    cells = cx * plane
    chunk = 2 * cz if cells % (2 * cz) == 0 else cz
    for first in range(0, cells, chunk):
        padded[first:first + chunk] = flat[first:first + chunk].astype(F32)
    row = lax.broadcasted_iota(jnp.int32, (cz, cz), 0)
    column = lax.broadcasted_iota(jnp.int32, (cz, cz), 1)
    zero_row = jnp.zeros((1, bands), F32)

    def segment(x, y):
        at = x * plane + y * cz
        centre = padded[at:at + cz]
        near = jnp.concatenate([zero_row, centre[:-1]]) + jnp.concatenate([centre[1:], zero_row])
        for there, offset in ((x > 0, -plane), (x < cx - 1, plane), (y > 0, -cz), (y < cy - 1, cz)):
            if there:
                near = near + padded[at + offset:at + offset + cz]
        local = jnp.broadcast_to(pot[y, x:x + 1, :], (cz, cz))
        factor = 3.0 + jnp.sum(jnp.where(row == column, local, 0.0), axis=1, keepdims=True)
        return factor * centre - 0.5 * near

    order = list(itertools.product(range(cx), range(cy)))
    per = chunk // cz
    for first in range(0, len(order), per):
        hq[first * cz:(first + per) * cz] = jnp.concatenate(
            [segment(*xy) for xy in order[first:first + per]]).astype(BF16)

    context = types.SimpleNamespace(
        copies=copies, sizes=sizes, digits=digits, strides=strides, peer=peer, gx=gx, partner=partner,
        parity=parity, rows=rows, half=half)
    taken = iter(buffers)

    scale = 1.0 / (cells * gyz_size)

    def streams(plan, source, final, both):
        return [Stream(context, source, final, both, first, last, order, [[next(taken) for _ in range(5)] for _ in order])
                for first, last, order in plan]

    ham_streams, corr_streams = streams(ham_plan, sum_h, ham_out, direct), streams(corr_plan, sum_c, corr_out, False)

    def begin(group):
        for stream in group:
            stream.start()

    def end(group):
        for stream in group:
            if stream.phase == len(stream.order):
                continue
            if stream.both and stream.phase == len(stream.order) - 1:
                stream.finish_both((mine, other), scale)
                continue
            stream.finish()
            if stream.both and stream.phase == len(stream.order) - 1:
                stream.start_both()
            elif stream.phase < len(stream.order):
                stream.start()

    with scope('pair_c'):
        pair_copy_c.wait_recv()
    sum_c[...] = corr[everything + (mine,)] + pair_c[...]
    begin(corr_streams)

    def corr_step():
        at = corr_streams[0].phase
        with scope("corr_%d" % at):
            end(corr_streams)

    for first in range(0, bands, tile):
        store_rows(ham, first, gram_t(flat[:, first:first + tile], hq[...]))

    def add_cross(target, column, value):
        for j in range(bands // rows):
            index = block_index(j) + (slice(None), column)
            target[index] = target[index] - 0.5 * value[j * rows:(j + 1) * rows]

    faces = []
    for at, (cells_x, y) in enumerate(((range(cut_x), 0), (range(cut_x, cx), cy - 1))):
        own = jnp.concatenate([flat[x * plane + y * cz:x * plane + y * cz + cz] for x in cells_x])
        face[at, 0:own.shape[0]] = own
        turned[at, :, 0:own.shape[0]] = jnp.transpose(own)
        faces.append((face.at[at, 0:own.shape[0]], turned.at[at, :, 0:own.shape[0]]))

    @pl.when(jnp.logical_not(first_x))
    def _():
        to_x.wait_recv()

    near, far = flat[0:plane], jnp.concatenate([halo_x[y] for y in range(cy)])
    for first in range(0, bands, tile):
        cut = slice(first, first + tile)
        add_cross(ham, cut, gram_t(near, far[:, cut]) + gram_t(far, near[:, cut]))

    with scope('ahead'):
        @pl.when(jnp.logical_not(first_y))
        def _():
            ahead.wait_recv()

    ghosts[0:cut_x * cz] = jnp.concatenate([halo_f[x] for x in range(cut_x)])
    forward = ghosts.at[0:cut_x * cz]
    forward_t = jnp.transpose(forward[...])
    backward = ghosts.at[cut_x * cz:cx * cz]

    def cross(at, ghost, ghost_t, column):
        near, near_t = faces[at]
        return (jnp.dot(near_t[...], ghost[:, column], preferred_element_type=F32)
                + jnp.dot(ghost_t, near[:, column], preferred_element_type=F32))

    def add(column, value):
        add_cross(ham, column, value)

    add(other, cross(0, forward, forward_t, other))
    pair_copy_h = copies.start(ham.at[everything + (other,)], pair_h, (partner, gyz))
    add(mine, cross(0, forward, forward_t, mine))

    if coef_state[0] < coef_steps:
        coef_step()
    with scope('back'):
        @pl.when(jnp.logical_not(last_y))
        def _():
            back.wait_recv()

    if coef_state[0] < coef_steps:
        coef_step()
    ghosts[cut_x * cz:cx * cz] = jnp.concatenate([halo_b[x] for x in range(cx - cut_x)])
    backward_t = jnp.transpose(backward[...])
    value = cross(1, backward, backward_t, other)
    for j in range(bands // rows):
        late[block_index(j)] = (-0.5 * value[j * rows:(j + 1) * rows]).astype(BF16)
    pieces = [(ham_streams[0], k, at) for k, at in enumerate(ham_streams[0].index(values) for _, values in ham_streams[0].peers())]
    pieces = [(stream, None, everything[:-1]) for stream in ham_streams[1:]] + [pieces[k] for k in far_first(ham_streams[0].order[0], len(pieces))] + pieces[:1]
    pair_copies_h = []
    for stream, k, at in pieces:
        at = at + (stream.rows,)
        pair_copies_h.append(copies.start(late.at[at], pair_l.at[at], (partner, gyz)))
    add(mine, cross(1, backward, backward_t, mine))
    with scope('pair_h'):
        ham_streams[0].open()
        pair_copy_h.wait_recv()
        for (stream, k, at), copy in zip(pieces, pair_copies_h):
            at = at + (stream.rows,)
            copy.wait_recv()
            sum_h[at] = ham[at + (mine,)] + pair_h[at] + pair_l[at].astype(F32)
            if k is None:
                stream.start()
            elif k:
                stream.send(k)

    def last_sum(group, gx_recv, final):
        total, others = group[0].source, []
        for k in range(1, gx_size // 2):
            target = (lax.rem(gx + 2 * k, gx_size), gyz)
            others.append(copies.start(total, gx_recv.at[k - 1], target))
        for copy in others:
            copy.wait_recv()
        total = total[...]
        for k in range(1, gx_size // 2):
            total = total + gx_recv[k - 1]
        final[:, mine] = total * scale
        return copies.start(final.at[:, mine], final.at[:, mine], (partner, gyz))

    part = max(size for size in range(16, 512, 16) if cells % size == 0)

    def rotate(column):
        some = coef[everything + (column,)].reshape(bands, half)
        for first in range(0, cells, part):
            rot_out[first:first + part, column] = jnp.dot(
                flat[first:first + part], some, preferred_element_type=F32).astype(BF16)

    last = []
    if relayed:
        steps = ["coef", "corr", "ham", "coef", "corr", "rot", "ham"]
    else:
        steps = ["coef"] * (coef_steps - coef_state[0]) + ["rot"]
        steps += ["corr"] * len(corr_plan[0][2]) + ["ham"] * len(ham_plan[0][2])
    for step in steps:
        if step == "corr":
            corr_step()
            if corr_streams[0].phase == len(corr_streams[0].order):
                last += [last_sum(corr_streams, gx_c, corr_out)]
        if step == "ham":
            at = ham_streams[0].phase
            for which, stream in enumerate(ham_streams):
                with scope("ham%d_%d" % (which, at)):
                    end([stream])
            if ham_streams[0].phase == len(ham_streams[0].order):
                last += [] if direct else [last_sum(ham_streams, gx_h, ham_out)]
        if step == "coef":
            coef_step()
        if step == "rot":
            rotate(mine)
            with scope("pair_e"):
                coef_state[2].wait_recv()
            rotate(other)
    with scope('last'):
        for copy in last:
            copy.wait_recv()
    copies.wait_sends()

    @pl.when(jnp.logical_not(last_y))
    def _():
        ahead.wait_send()

    @pl.when(jnp.logical_not(first_y))
    def _():
        back.wait_send()

    @pl.when(jnp.logical_not(last_x))
    def _():
        to_x.wait_send()

    assert copies.used == copy_count


def deliver(corr, ham, rot, corr_out, ham_out, rot_out, sems):
    copies = [pltpu.make_async_copy(source, target, sems.at[i]) for i, (source, target) in
              enumerate(((rot, rot_out), (corr, corr_out), (ham, ham_out)))]
    for copy in copies:
        copy.start()
    for copy in copies:
        copy.wait()


def in_hbm(array):
    return pltpu.with_memory_space_constraint(array, pltpu.HBM)


def on_device(bands, potential, eigenvectors):
    gx_size, gyz_size = lax.axis_size("gx"), lax.axis_size("gyz")
    cx, cy, cz, width = bands.shape
    rows = eigenvectors.shape[0]
    cells = cx * cy * cz
    sizes = digit_sizes(gyz_size)
    count = len(sizes)
    half = width // 2
    flat = bands.reshape(cells, width)
    ham_plan, corr_plan, coef_plan = plans_of(rows, sizes)
    copy_count = 4 + peer_count(sizes, ham_plan[0][2][0]) + len(ham_plan) - 1
    copy_count += sum(len(order) for _, _, order in ham_plan + corr_plan)
    copy_count += len(coef_plan) + 2 * (sizes == (2, 2, 2, 2)) - 1
    copy_count += 1 if gx_size == 2 else 2 * (gx_size // 2)
    geometry = (gx_size, gyz_size, cx, cy, cz, width, rows, sizes, copy_count)

    buffers = []
    for at, (first, last, order) in enumerate(ham_plan + corr_plan):
        left = list(range(count))
        for group in order:
            many = peer_count(sizes, group)
            many = 2 * many - 1 if gx_size == 2 and at < len(ham_plan) and group == order[-1] else many - 1
            whole, spots = tuple(sizes[i] for i in left), tuple(sizes[i] for i in left if i in group)
            left = [d for d in left if d not in group]
            kept = tuple(sizes[i] for i in left)
            cut, lines = (last - first, half), (math.prod(kept), half)
            buffers += [pltpu.VMEM(whole + cut, BF16), pltpu.VMEM(spots + lines, F32),
                        pltpu.VMEM((many,) + kept + cut, BF16), pltpu.VMEM((many,) + lines, F32),
                        pltpu.VMEM(kept + cut, F32)]

    cut_x = (cx + 1) // 2
    wide, narrow = sizes + (rows, width), sizes + (rows, half)
    others = max(gx_size // 2 - 1, 1)
    vmem, anywhere = pl.BlockSpec(memory_space=pltpu.VMEM), pl.BlockSpec(memory_space=pl.ANY)
    results = (jax.ShapeDtypeStruct((rows, width), F32), jax.ShapeDtypeStruct((rows, width), F32),
               jax.ShapeDtypeStruct((cells, width), BF16))
    computed = pl.pallas_call(
        functools.partial(kernel, geometry),
        out_shape=results,
        in_specs=[pl.BlockSpec(memory_space=pltpu.HBM)] * 4,
        out_specs=(vmem, vmem, vmem),
        scratch_shapes=[
            pltpu.VMEM((cells, width), BF16), pltpu.VMEM((cy, cx, cz), F32),
            pltpu.VMEM(wide, BF16),
            pltpu.VMEM((cells, width), F32), pltpu.VMEM((cells, width), BF16),
            pltpu.VMEM(wide, F32), pltpu.VMEM(wide, F32),
            pltpu.VMEM((cut_x, cz, width), BF16), pltpu.VMEM((cx - cut_x, cz, width), BF16),
            pltpu.VMEM((cy, cz, width), BF16),
            pltpu.VMEM((2, cut_x * cz, width), BF16), pltpu.VMEM((2, width, cut_x * cz), BF16),
            pltpu.VMEM((cx * cz, width), BF16), pltpu.VMEM(narrow, BF16), pltpu.VMEM(narrow, BF16),
            pltpu.VMEM(narrow, F32), pltpu.VMEM(narrow, F32),
            pltpu.VMEM(narrow, F32), pltpu.VMEM(narrow, F32),
            pltpu.VMEM((others, rows, half), F32), pltpu.VMEM((others, rows, half), F32),
            pltpu.VMEM((cells * width // 1024, 8, 128), F32), pltpu.VMEM((256, 1, half), F32),
            pltpu.SemaphoreType.DMA((5,)), pltpu.SemaphoreType.DMA((copy_count + 3,)),
            pltpu.SemaphoreType.DMA((3,)), *buffers,
        ],
        compiler_params=pltpu.CompilerParams(
            collective_id=0, has_side_effects=True, vmem_limit_bytes=52 * 1024 * 1024),
    )(bands, flat, in_hbm(jnp.transpose(potential, (1, 0, 2))), in_hbm(eigenvectors))
    corr, ham, rotated = pl.pallas_call(
        deliver, out_shape=results, in_specs=[vmem] * 3, out_specs=[anywhere] * 3,
        scratch_shapes=[pltpu.SemaphoreType.DMA((3,))],
        compiler_params=pltpu.CompilerParams(vmem_limit_bytes=8 * 1024 * 1024),
    )(*computed)
    return corr, ham, rotated.reshape(bands.shape)


def solution(mesh):
    in_specs = (P("gx", "gyz", None, None), P("gx", "gyz", None), P("gyz", None))
    out_specs = (P("gyz", None), P("gyz", None), P("gx", "gyz", None, None))
    return jax.shard_map(
        on_device, mesh=mesh, in_specs=in_specs, out_specs=out_specs, check_vma=False
    )
```
